32 devices in a mesh: row: 8 (over z, x), col: 4 (over y, core).
Axes of the slice: x: 2, y: 2, z: 4, core: 2. Of those that a mesh axis runs over, the one named last changes fastest.
Arguments:
- dense_a: bfloat16 [64, 512, 512], P(('row', 'col')), may hold values from -6 to 6
- dense_b: bfloat16 [64, 512, 512], P(('row', 'col')), may hold values from -0.25 to 0.25
- inner_basis_stack: bfloat16 [64, 2, 512, 128], P(('row', 'col')), may hold values from -0.25 to 0.25
- outer_basis_stack: bfloat16 [64, 2, 512, 128], P(('row', 'col')), may hold values from -1 to 1
- ascent: bfloat16 [32, 4, 2, 128, 128], P(('row', 'col')), may hold values from -0.4375 to 0.4375
- descent: bfloat16 [32, 4, 2, 128, 128], P(('row', 'col')), may hold values from -0.5 to 0.5
- couplings: bfloat16 [32, 2, 4, 128, 128], P(('row', 'col')), may hold values from -0.5 to 0.5
Outputs:
- product_diag: bfloat16 [64, 512, 512], P(('row', 'col'))
The draws below stay inside these ranges and needn't reach their ends.
All inputs are finite; a program needn't handle non-finite values.
Results may differ from the reference program's by a relative error of at most 0.015.
Values may be sent and summed in bfloat16 or wider, within the bound.
A program may use at most 64 MiB of HBM per device.

```python
import jax
import jax.numpy as jnp
from jax import lax

M = 512
R = 128
DEVICES_ALL = 32
LEAVES = 64
N_ROW = 8
N_COL = 4


def block_scale(rng, extent, shards, low, largest):
    level, own = 1.0, jax.random.fold_in(rng, 6)
    for position, shards_of in shards:
        draws = jnp.exp(jax.random.uniform(jax.random.fold_in(own, position), (shards_of,), jnp.float32, low / len(shards), largest / len(shards)))
        level = level * jnp.repeat(draws, extent[position] // shards_of).reshape([-1 if axis == position else 1 for axis in range(len(extent))])
    return level


def scatter_about(own_key, dims, width, reach, shards=(), kind=jnp.bfloat16):
    factor_of = block_scale(own_key, dims, shards, -0.22, 0.18) if shards else 1.0
    drawn = jax.random.normal(own_key, dims, jnp.float32) * width * factor_of
    return jnp.minimum(jnp.maximum(drawn, -reach), reach).astype(kind)


def setup_inputs(seed: int = 0) -> dict:
    keys = jax.random.split(jax.random.key(seed), 8)
    dense_a = scatter_about(keys[0], (LEAVES, M, M), 1.0, 6.0, ((0, 32),))
    dense_b = scatter_about(keys[1], (LEAVES, M, M), M ** -0.5, 0.25, ((0, 32),))
    inner_basis_stack = scatter_about(keys[2], (LEAVES, 2, M, R), M ** -0.5, 0.25, ((0, 32),))
    outer_basis_stack = scatter_about(keys[3], (LEAVES, 2, M, R), (R // 4) ** -0.5, 1.0, ((0, 32),))
    ascent = scatter_about(keys[4], (DEVICES_ALL, 4, 2, R, R), (R * 7 // 5) ** -0.5, 0.4375, ((0, 32),))
    descent = scatter_about(keys[5], (DEVICES_ALL, 4, 2, R, R), R ** -0.5, 0.5, ((0, 32),))
    couplings = scatter_about(keys[6], (DEVICES_ALL, 2, 4, R, R), R ** -0.5, 0.5, ((0, 32),))
    return {"dense_a": dense_a, "dense_b": dense_b, "inner_basis_stack": inner_basis_stack, "outer_basis_stack": outer_basis_stack, "ascent": ascent, "descent": descent, "couplings": couplings}


HIGHEST_PRECISION = lax.Precision.HIGHEST


def multiply(first_arg, second_arg):
    return jnp.matmul(first_arg.astype(jnp.float32), second_arg.astype(jnp.float32), precision=HIGHEST_PRECISION)


def lifted(pair_stack, inner_value):
    return multiply(multiply(jnp.swapaxes(pair_stack[:, 0], 1, 2), inner_value), pair_stack[:, 1])


def lowered(pair_stack, parent):
    return multiply(multiply(pair_stack[:, 0], parent), jnp.swapaxes(pair_stack[:, 1], 1, 2))


def sibling_terms(blocks, inner_value):
    left_terms = multiply(multiply(blocks[:, 0], inner_value[1::2]), blocks[:, 3])
    right_terms = multiply(multiply(blocks[:, 1], inner_value[0::2]), blocks[:, 2])
    return jnp.stack([left_terms, right_terms], 1).reshape(inner_value.shape)


def owners(stacked, height):
    return stacked[2 ** (height - 1) - 1::2 ** height]


def leaf_block(leaf_items):
    first_matrix_block, block_b, bases, mixing = leaf_items
    spread_rows = jnp.dot(bases[0], mixing, preferred_element_type=jnp.float32).astype(jnp.bfloat16)
    result_block = jnp.dot(first_matrix_block, block_b, preferred_element_type=jnp.float32)
    result_block = result_block + jnp.dot(spread_rows, bases[1].T, preferred_element_type=jnp.float32)
    return result_block.astype(jnp.bfloat16)


def reference(dense_a, dense_b, inner_basis_stack, outer_basis_stack, ascent, descent, couplings):
    device_list = N_ROW * N_COL
    levels = device_list.bit_length() - 1
    leaf_inner_product = jnp.einsum('ufw,ufa->uwa', inner_basis_stack[:, 0].astype(jnp.float32),
                            inner_basis_stack[:, 1].astype(jnp.float32), precision=HIGHEST_PRECISION)
    leaf_up = ascent[:, 0:2].reshape(2 * device_list, 2, R, R)
    inner_levels = [leaf_inner_product]
    lifted_terms = lifted(leaf_up, leaf_inner_product)
    current = lifted_terms[0::2] + lifted_terms[1::2]
    inner_levels.append(current)
    for height in range(1, levels + 1):
        if height == 1:
            pair_stack = ascent[:, 2]
        else:
            pair_stack = owners(ascent[:, 3], height - 1)
        lifted_terms = lifted(pair_stack, current)
        current = lifted_terms[0::2] + lifted_terms[1::2]
        inner_levels.append(current)
    coupling = jnp.zeros((1, R, R), jnp.float32)
    for height in range(levels, 0, -1):
        near_terms = sibling_terms(owners(couplings[:, 1], height), inner_levels[height])
        if height == 1:
            pair_stack = descent[:, 2]
        else:
            pair_stack = owners(descent[:, 3], height - 1)
        coupling = near_terms + lowered(pair_stack, jnp.repeat(coupling, 2, axis=0))
    near_terms = sibling_terms(couplings[:, 0], leaf_inner_product)
    leaf_down = descent[:, 0:2].reshape(2 * device_list, 2, R, R)
    leaf_coupling = near_terms + lowered(leaf_down, jnp.repeat(coupling, 2, axis=0))
    rounded_count = leaf_coupling.astype(jnp.bfloat16)
    return lax.map(leaf_block, (dense_a, dense_b, outer_basis_stack, rounded_count))
```

```python
import functools

import jax
import jax.numpy as jnp
from jax import lax
from jax.experimental import pallas as pl
from jax.experimental.pallas import tpu as pltpu
from jax.sharding import PartitionSpec as P

MESH = pl.DeviceIdType.MESH
BF16 = jnp.bfloat16
F32 = jnp.float32
ASC, DESC, COUP, SIB = 0, 1, 2, 3


def mm(a, b, ca=1, cb=0):
    return lax.dot_general(
        a.astype(BF16), b.astype(BF16), (((ca,), (cb,)), ((), ())), preferred_element_type=F32
    )


def rows(values):
    return jnp.concatenate([v.astype(BF16) for v in values], 0)


def cols(values):
    return jnp.concatenate([v.astype(BF16) for v in values], 1)


def split(levels):
    cuts = [0, 1]
    while cuts[-1] < levels:
        cuts.append(min(cuts[-1] + 2, levels))
    return list(zip(cuts[:-1], cuts[1:]))


def tree_kernel(
    levels, columns,
    da_ref, db_ref, inner_ref, outer_ref, asc_ref, desc_ref, coup_ref, o_ref,
    da, db, inner, outer, asc, desc, coup, base, left, right,
    table, t_out, n_out, t_in, n_in,
    load_sem, w_send, w_recv, t_send, t_recv, n_send, n_recv,
):
    pos = lax.axis_index("row") * columns + lax.axis_index("col")
    bit = [pos // 2**i % 2 for i in range(levels)]
    groups = split(levels)
    final = len(groups) - 1
    top = {h: g for g, (lo, hi) in enumerate(groups) for h in range(lo + 1, hi + 1)}
    late = list(range(groups[final][0] + 1, levels + 1))
    r = asc.shape[-1]

    def neighbour(g, f):
        lo, hi = groups[g]
        other = pos
        for i in range(lo, hi):
            if f >> (i - lo) & 1:
                other = other + 2**i * (1 - 2 * bit[i])
        return other // columns, other % columns

    def flips(g):
        lo, hi = groups[g]
        return list(reversed(range(1, 2 ** (hi - lo))))

    def ones(n):
        return pos % 2**n == 2**n - 1

    def owner(h):
        return pos % 2**h == 2 ** (h - 1) - 1

    barrier = pltpu.get_barrier_semaphore()
    greeted = [neighbour(g, f) for g in range(final + 1) for f in flips(g)]
    for other in greeted:
        pl.semaphore_signal(barrier, inc=1, device_id=other, device_id_type=MESH)

    loads = [
        pltpu.make_async_copy(src, dst, load_sem.at[n])
        for n, (src, dst) in enumerate([
            (asc_ref.at[0], asc),
            (inner_ref, inner),
            (coup_ref.at[0], coup),
            (desc_ref.at[0], desc),
            (da_ref, da),
            (db_ref, db),
            (outer_ref, outer),
        ])
    ]
    for copy in loads[:4]:
        copy.start()

    def slot(kind, h):
        return table.at[kind, h]

    def targets(kind, h, g):
        lo, _ = groups[g]
        if g < top[h]:
            return [(f, kind, slot(kind, h)) for f in flips(g)]
        found = []
        for f in flips(g):
            beyond = f >> (h - lo)
            if kind == ASC:
                found.append((f, SIB if beyond else ASC, slot(ASC, h)))
            elif beyond:
                continue
            elif kind == COUP and f >> (h - 1 - lo) & 1:
                found.append((f, COUP, coup.at[1, 1:3]))
            else:
                found.append((f, kind, slot(kind, h)))
        return found

    def copies(kind, h, g):
        return [
            pltpu.make_async_remote_copy(
                src_ref=src, dst_ref=slot(to, h),
                send_sem=w_send.at[kind, h, g, f - 1], recv_sem=w_recv.at[to, h],
                device_id=neighbour(g, f), device_id_type=MESH,
            )
            for f, to, src in targets(kind, h, g)
        ]

    def give(kind, h, gs):
        @pl.when(owner(h))
        def _():
            for g in gs:
                for copy in copies(kind, h, g):
                    copy.start()

    def down(h):
        return list(reversed(range(top[h] + 1)))

    def take(kind, h, who=None):
        waits = jnp.logical_not(owner(h)) if kind != SIB else None
        if who is not None:
            waits = who if waits is None else waits & who

        def body():
            pltpu.make_async_copy(slot(kind, h), slot(kind, h), w_recv.at[kind, h]).wait()
            for g in reversed(range(top[h])):
                @pl.when(ones(groups[g][1]))
                def _(g=g):
                    for copy in copies(kind, h, g):
                        copy.start()

        if waits is None:
            body()
        else:
            pl.when(waits)(body)

    def t_copy(g, f):
        return pltpu.make_async_remote_copy(
            src_ref=t_out.at[g], dst_ref=t_in.at[g, f - 1],
            send_sem=t_send.at[g, f - 1], recv_sem=t_recv.at[g, f - 1],
            device_id=neighbour(g, f), device_id_type=MESH,
        )

    def n_copy(g):
        return pltpu.make_async_remote_copy(
            src_ref=n_out.at[g], dst_ref=n_in.at[g],
            send_sem=n_send.at[g], recv_sem=n_recv.at[g],
            device_id=neighbour(g, 1), device_id_type=MESH,
        )

    sends_next = jnp.logical_not(ones(1))
    relay = ones(1)

    loads[0].wait()
    turned = cols([asc[u, 0].T for u in range(2)])
    lifted_left = mm(asc[2, 0].T, turned).astype(BF16)
    lifted_right = mm(rows([asc[u, 1] for u in range(2)]), asc[2, 1])
    factors = [cols([asc[u, 1], lifted_right[u * r:(u + 1) * r]]) for u in range(2)]
    loads[1].wait()
    for copy in loads[4:]:
        copy.start()
    leaf = [mm(inner[u, 0], inner[u, 1], 0, 0).astype(BF16) for u in range(2)]
    half = rows([mm(leaf[u], factors[u]) for u in range(2)])
    term = mm(lifted_left, half[:, r:])
    t_out[0] = term.astype(BF16)
    n_out[0] = mm(turned, half[:, :r]).astype(BF16)

    loads[2].wait()
    loads[3].wait()
    for h in range(1, levels + 1):
        @pl.when(owner(h))
        def _(h=h):
            table[COUP, h, 0] = coup[1, 0]
            table[COUP, h, 1] = coup[1, 3]
            if h < levels - 1:
                table[ASC, h, 0] = asc[3, 0].T
                table[ASC, h, 1] = asc[3, 1]
                table[DESC, h] = desc[3]

    pl.semaphore_wait(barrier, len(greeted))
    t_copy(0, 1).start()
    n_copy(0).start()
    for h in range(1, levels - 1):
        give(ASC, h, down(h))
    for h in reversed(late):
        give(COUP, h, [final])

    near = [
        mm(mm(coup[0, 0], leaf[1]), coup[0, 3]),
        mm(mm(coup[0, 1], leaf[0]), coup[0, 2]),
    ]
    left_chain = rows([desc[u, 0] for u in range(2)])
    right_chain = rows([desc[u, 1] for u in range(2)])

    t_copy(0, 1).wait()
    node = term + t_in[0, 0].astype(F32)
    crossed = {}
    for g in range(1, final + 1):
        lo, hi = groups[g]
        n_out[g] = node.astype(BF16)
        if hi - lo == 2:
            take(ASC, lo, None if g == 1 else sends_next)
            term = mm(table[ASC, lo, 0], mm(node, table[ASC, lo, 1]))
            t_out[g] = term.astype(BF16)
            for f in flips(g):
                if g < final or f > 1:
                    t_copy(g, f).start()
        n_copy(g).start()
        if g == 1:
            for h in range(1, levels - 1):
                give(COUP, h, down(h))
                give(DESC, h, down(h))
            for h in late:
                give(COUP, h, down(h)[1:])
            loads[4].wait()
            loads[5].wait()
            for u in range(2):
                base[u] = mm(da[u], db[u])
            for h in range(2, levels - 1):
                take(ASC, h, relay)
                if h == groups[top[h]][0] + 1:
                    take(SIB, h, relay)
            for h in late:
                take(COUP, h, ones(groups[final][0]))
        if g < final:
            for f in flips(g):
                t_copy(g, f).wait()
            own = (term + t_in[g, 0].astype(F32)).astype(BF16)
            other = (t_in[g, 1].astype(F32) + t_in[g, 2].astype(F32)).astype(BF16)
            crossed[lo + 2] = other
            take(ASC, lo + 1, sends_next)
            take(SIB, lo + 1, sends_next)
            node = mm(
                cols([table[ASC, lo + 1, 0], table[SIB, lo + 1, 0]]),
                rows([mm(own, table[ASC, lo + 1, 1]), mm(other, table[SIB, lo + 1, 1])]),
            )

    loads[6].wait()
    for h in range(1, levels + 1):
        if h == 2:
            left_chain = mm(left_chain, desc[2, 0]).astype(BF16)
            right_chain = mm(right_chain, desc[2, 1]).astype(BF16)
        elif h > 2:
            take(DESC, h - 2)
            left_chain = mm(left_chain, table[DESC, h - 2, 0]).astype(BF16)
            right_chain = mm(right_chain, table[DESC, h - 2, 1]).astype(BF16)
        if h in late:
            take(COUP, h, jnp.logical_not(ones(groups[final][0])))
        else:
            take(COUP, h)
        before = mm(left_chain, table[COUP, h, 0]).astype(BF16)
        after = mm(table[COUP, h, 1], right_chain, 1, 1).astype(BF16)
        if h in late:
            at = late.index(h) * r
            for u in range(2):
                left[u, :, at:at + r] = mm(outer[u, 0], before[u * r:(u + 1) * r]).astype(BF16)
                right[u, at:at + r, :] = mm(after[:, u * r:(u + 1) * r], outer[u, 1], 1, 1).astype(BF16)
        else:
            if h == groups[top[h]][0] + 1:
                n_copy(top[h]).wait()
                value = n_in[top[h]]
            else:
                value = crossed[h]
            spread = mm(value, after).astype(BF16)
            for u in range(2):
                near[u] += mm(before[u * r:(u + 1) * r], spread[:, u * r:(u + 1) * r])
        if h == late[0] - 1:
            for u in range(2):
                base[u] += mm(mm(outer[u, 0], near[u]), outer[u, 1], 1, 1)

    n_copy(final).wait()
    blocks = [n_in[final]]
    if len(late) == 2:
        for f in (2, 3):
            t_copy(final, f).wait()
        blocks.append((t_in[final, 1].astype(F32) + t_in[final, 2].astype(F32)).astype(BF16))
        zero = jnp.zeros_like(blocks[0])
        blocks = rows([cols([blocks[0], zero]), cols([zero, blocks[1]])])
    else:
        blocks = blocks[0]
    for u in range(2):
        o_ref[u] = (base[u] + mm(mm(left[u], blocks), right[u])).astype(BF16)

    for h in range(1, levels + 1):
        for kind in (ASC, SIB, DESC, COUP):
            if kind != COUP and h > levels - 2:
                continue
            if kind == SIB and (h == 1 or h != groups[top[h]][0] + 1):
                continue
            for g in range(top[h] + 1):
                if g == top[h] and kind == SIB:
                    continue

                @pl.when(owner(h) if g == top[h] else ones(groups[g][1]))
                def _(kind=kind, h=h, g=g):
                    for copy in copies(kind, h, g):
                        copy.wait_send()


def shards(levels, columns, dense_a, dense_b, inner, outer, ascent, descent, couplings):
    r = ascent.shape[-1]
    m = dense_a.shape[-1]
    arrays = (dense_a, dense_b, inner, outer, ascent, descent, couplings)
    vmem = pltpu.VMEM
    dma = pltpu.SemaphoreType.DMA
    groups = split(levels)
    n = len(groups)
    wide = groups[-1][1] - groups[-1][0]
    return pl.pallas_call(
        functools.partial(tree_kernel, levels, columns),
        out_shape=jax.ShapeDtypeStruct(dense_a.shape, BF16),
        in_specs=[pl.BlockSpec(memory_space=pltpu.HBM)] * 7,
        out_specs=pl.BlockSpec(memory_space=pltpu.VMEM),
        scratch_shapes=[
            vmem(dense_a.shape, BF16),
            vmem(dense_b.shape, BF16),
            vmem(inner.shape, BF16),
            vmem(outer.shape, BF16),
            vmem(ascent.shape[1:], BF16),
            vmem(descent.shape[1:], BF16),
            vmem(couplings.shape[1:], BF16),
            vmem(dense_a.shape, F32),
            vmem((2, m, wide * r), BF16),
            vmem((2, wide * r, m), BF16),
            vmem((4, levels + 1, 2, r, r), BF16),
            vmem((n, r, r), BF16),
            vmem((n, r, r), BF16),
            vmem((n, 3, r, r), BF16),
            vmem((n, r, r), BF16),
            dma((7,)),
            dma((4, levels + 1, n, 3)),
            dma((4, levels + 1)),
            dma((n, 3)),
            dma((n, 3)),
            dma((n,)),
            dma((n,)),
        ],
        compiler_params=pltpu.CompilerParams(collective_id=0, has_side_effects=True, vmem_limit_bytes=24 * 2**20),
    )(*(pltpu.with_memory_space_constraint(x, pltpu.HBM) for x in arrays))


def solution(mesh):
    rows_, columns = mesh.shape["row"], mesh.shape["col"]
    levels = (rows_ * columns).bit_length() - 1
    both = ("row", "col")
    placed = (
        P(both, None, None),
        P(both, None, None),
        P(both, None, None, None),
        P(both, None, None, None),
        P(both, None, None, None, None),
        P(both, None, None, None, None),
        P(both, None, None, None, None),
    )
    return jax.shard_map(
        functools.partial(shards, levels, columns),
        mesh=mesh, in_specs=placed, out_specs=P(both, None, None), check_vma=False,
    )
```

```python
import functools

import jax
import jax.numpy as jnp
from jax import lax
from jax.experimental import pallas as pl
from jax.experimental.pallas import tpu as pltpu
from jax.sharding import PartitionSpec as P

MESH = pl.DeviceIdType.MESH
BF16 = jnp.bfloat16
F32 = jnp.float32
ASC, DESC, COUP, SIB = 0, 1, 2, 3


def mm(a, b, ca=1, cb=0):
    return lax.dot_general(
        a.astype(BF16), b.astype(BF16), (((ca,), (cb,)), ((), ())), preferred_element_type=F32
    )


def rows(values):
    return jnp.concatenate([v.astype(BF16) for v in values], 0)


def cols(values):
    return jnp.concatenate([v.astype(BF16) for v in values], 1)


def split(levels):
    cuts = [0, 1]
    while cuts[-1] < levels:
        cuts.append(min(cuts[-1] + 2, levels))
    return list(zip(cuts[:-1], cuts[1:]))


def kept(levels):
    groups = split(levels)
    firsts = [lo + 1 for lo, hi in groups[1:-1] if hi - lo == 2]
    found = [(COUP, h) for h in range(1, levels + 1)]
    found += [(kind, h) for h in range(1, levels - 1) for kind in (ASC, DESC)]
    return found + [(SIB, h) for h in firsts]


def tree_kernel(
    levels, columns,
    da_ref, db_ref, inner_ref, outer_ref, asc_ref, desc_ref, coup_ref, o_ref,
    da, db, inner, outer, asc, desc, coup, base, left, right,
    table, t_out, n_out, d_in,
    load_sem, w_send, w_recv, d_send, d_recv,
):
    pos = lax.axis_index("row") * columns + lax.axis_index("col")
    bit = [pos // 2**i % 2 for i in range(levels)]
    groups = split(levels)
    final = len(groups) - 1
    top = {h: g for g, (lo, hi) in enumerate(groups) for h in range(lo + 1, hi + 1)}
    late = list(range(groups[final][0] + 1, levels + 1))
    r, m = asc.shape[-1], da.shape[-1]
    place = {item: n for n, item in enumerate(kept(levels))}

    def neighbour(g, f):
        lo, hi = groups[g]
        other = pos
        for i in range(lo, hi):
            if f >> (i - lo) & 1:
                other = other + 2**i * (1 - 2 * bit[i])
        return other // columns, other % columns

    def flips(g):
        lo, hi = groups[g]
        return list(reversed(range(1, 2 ** (hi - lo))))

    def ones(n):
        return pos % 2**n == 2**n - 1

    def owner(h):
        return pos % 2**h == 2 ** (h - 1) - 1

    barrier = pltpu.get_barrier_semaphore()
    greeted = [neighbour(g, f) for g in range(final + 1) for f in flips(g)]
    for other in greeted:
        pl.semaphore_signal(barrier, inc=1, device_id=other, device_id_type=MESH)

    loads = [
        pltpu.make_async_copy(src, dst, load_sem.at[n])
        for n, (src, dst) in enumerate([
            (asc_ref.at[0], asc),
            (inner_ref, inner),
            (coup_ref.at[0], coup),
            (desc_ref.at[0], desc),
            (da_ref, da),
            (db_ref, db),
            (outer_ref, outer),
        ])
    ]
    for copy in loads[:4]:
        copy.start()

    def slot(kind, h):
        return table.at[place[kind, h]]

    def weight(kind, h, n):
        return table[place[kind, h], n]

    def targets(kind, h, g):
        lo, _ = groups[g]
        if g < top[h]:
            return [(f, kind, slot(kind, h)) for f in flips(g)]
        found = []
        for f in flips(g):
            beyond = f >> (h - lo)
            if kind == ASC:
                found.append((f, SIB if beyond else ASC, slot(ASC, h)))
            elif beyond:
                continue
            elif kind == COUP and f >> (h - 1 - lo) & 1:
                found.append((f, COUP, coup.at[1, 1:3]))
            else:
                found.append((f, kind, slot(kind, h)))
        return found

    def copies(kind, h, g):
        return [
            pltpu.make_async_remote_copy(
                src_ref=src, dst_ref=slot(to, h),
                send_sem=w_send.at[g], recv_sem=w_recv.at[place[to, h]],
                device_id=neighbour(g, f), device_id_type=MESH,
            )
            for f, to, src in targets(kind, h, g)
        ]

    def give(kind, h, gs):
        @pl.when(owner(h))
        def _():
            for g in gs:
                for copy in copies(kind, h, g):
                    copy.start()

    def down(h):
        return list(reversed(range(top[h] + 1)))

    def take(kind, h, who=None):
        waits = jnp.logical_not(owner(h)) if kind != SIB else None
        if who is not None:
            waits = who if waits is None else waits & who

        def body():
            pltpu.make_async_copy(slot(kind, h), slot(kind, h), w_recv.at[place[kind, h]]).wait()
            for g in reversed(range(top[h])):
                @pl.when(ones(groups[g][1]))
                def _(g=g):
                    for copy in copies(kind, h, g):
                        copy.start()

        if waits is None:
            body()
        else:
            pl.when(waits)(body)

    def arrival(g, f):
        return 2 * g if f or g == final else 2 * g + 1

    def d_copy(g, f):
        return pltpu.make_async_remote_copy(
            src_ref=(t_out if f else n_out).at[g], dst_ref=d_in.at[g, f - 1 if g == final and f else f],
            send_sem=d_send.at[g], recv_sem=d_recv.at[arrival(g, f)],
            device_id=neighbour(g, f or 1), device_id_type=MESH,
        )

    def arrived(g, start, stop):
        part = d_in.at[g, start:stop]
        pltpu.make_async_copy(part, part, d_recv.at[arrival(g, start)]).wait()

    sends_next = jnp.logical_not(ones(1))
    relay = ones(1)

    loads[0].wait()
    turned = cols([asc[u, 0].T for u in range(2)])
    lifted_left = mm(asc[2, 0].T, turned).astype(BF16)
    lifted_right = mm(rows([asc[u, 1] for u in range(2)]), asc[2, 1])
    factors = [cols([asc[u, 1], lifted_right[u * r:(u + 1) * r]]) for u in range(2)]
    loads[1].wait()
    for copy in loads[4:]:
        copy.start()
    leaf = [mm(inner[u, 0], inner[u, 1], 0, 0).astype(BF16) for u in range(2)]
    half = rows([mm(leaf[u], factors[u]) for u in range(2)])
    term = mm(lifted_left, half[:, r:])
    t_out[0] = term.astype(BF16)
    n_out[0] = mm(turned, half[:, :r]).astype(BF16)

    loads[2].wait()
    loads[3].wait()
    for h in range(1, levels + 1):
        @pl.when(owner(h))
        def _(h=h):
            table[place[COUP, h], 0] = coup[1, 0]
            table[place[COUP, h], 1] = coup[1, 3]
            if h < levels - 1:
                table[place[ASC, h], 0] = asc[3, 0].T
                table[place[ASC, h], 1] = asc[3, 1]
                table[place[DESC, h]] = desc[3]

    pl.semaphore_wait(barrier, len(greeted))
    d_copy(0, 1).start()
    d_copy(0, 0).start()
    for h in range(1, levels - 1):
        give(ASC, h, down(h))
    for h in reversed(late):
        give(COUP, h, [final])

    near = [
        mm(mm(coup[0, 0], leaf[1]), coup[0, 3]),
        mm(mm(coup[0, 1], leaf[0]), coup[0, 2]),
    ]
    left_chain = rows([desc[u, 0] for u in range(2)])
    right_chain = rows([desc[u, 1] for u in range(2)])

    arrived(0, 1, 2)
    node = term + d_in[0, 1].astype(F32)
    crossed = {}
    for g in range(1, final + 1):
        lo, hi = groups[g]
        n_out[g] = node.astype(BF16)
        if hi - lo == 2:
            take(ASC, lo, None if g == 1 else sends_next)
            term = mm(weight(ASC, lo, 0), mm(node, weight(ASC, lo, 1)))
            t_out[g] = term.astype(BF16)
            for f in flips(g):
                if g < final or f > 1:
                    d_copy(g, f).start()
        d_copy(g, 0).start()
        if g == 1:
            for h in range(1, levels - 1):
                give(COUP, h, down(h))
                give(DESC, h, down(h))
            for h in late:
                give(COUP, h, down(h)[1:])
            loads[4].wait()
            loads[5].wait()
            for u in range(2):
                base[u * m:(u + 1) * m] = mm(da[u], db[u])
            for h in range(2, levels - 1):
                take(ASC, h, relay)
                if (SIB, h) in place:
                    take(SIB, h, relay)
            for h in late:
                take(COUP, h, ones(groups[final][0]))
        if g < final:
            arrived(g, 1, 4)
            own = (term + d_in[g, 1].astype(F32)).astype(BF16)
            other = (d_in[g, 2].astype(F32) + d_in[g, 3].astype(F32)).astype(BF16)
            crossed[lo + 2] = other
            take(ASC, lo + 1, sends_next)
            take(SIB, lo + 1, sends_next)
            node = mm(
                cols([weight(ASC, lo + 1, 0), weight(SIB, lo + 1, 0)]),
                rows([mm(own, weight(ASC, lo + 1, 1)), mm(other, weight(SIB, lo + 1, 1))]),
            )

    loads[6].wait()
    for h in range(1, levels + 1):
        if h == 2:
            left_chain = mm(left_chain, desc[2, 0]).astype(BF16)
            right_chain = mm(right_chain, desc[2, 1]).astype(BF16)
        elif h > 2:
            take(DESC, h - 2)
            left_chain = mm(left_chain, weight(DESC, h - 2, 0)).astype(BF16)
            right_chain = mm(right_chain, weight(DESC, h - 2, 1)).astype(BF16)
        if h in late:
            take(COUP, h, jnp.logical_not(ones(groups[final][0])))
        else:
            take(COUP, h)
        before = mm(left_chain, weight(COUP, h, 0)).astype(BF16)
        after = mm(weight(COUP, h, 1), right_chain, 1, 1).astype(BF16)
        if h in late:
            at = late.index(h) * r
            for u in range(2):
                left[u, :, at:at + r] = mm(outer[u, 0], before[u * r:(u + 1) * r]).astype(BF16)
                right[u, at:at + r, :] = mm(after[:, u * r:(u + 1) * r], outer[u, 1], 1, 1).astype(BF16)
        else:
            if h == groups[top[h]][0] + 1:
                arrived(top[h], 0, 1)
                value = d_in[top[h], 0]
            else:
                value = crossed[h]
            spread = mm(value, after).astype(BF16)
            for u in range(2):
                near[u] += mm(before[u * r:(u + 1) * r], spread[:, u * r:(u + 1) * r])
        if h == late[0] - 1:
            for u in range(2):
                base[u * m:(u + 1) * m] += mm(mm(outer[u, 0], near[u]), outer[u, 1], 1, 1)

    arrived(final, 0, 1 if len(late) == 1 else 3)
    blocks = [d_in[final, 0]]
    if len(late) == 2:
        blocks.append((d_in[final, 1].astype(F32) + d_in[final, 2].astype(F32)).astype(BF16))
        zero = jnp.zeros_like(blocks[0])
        blocks = rows([cols([blocks[0], zero]), cols([zero, blocks[1]])])
    else:
        blocks = blocks[0]
    for u in range(2):
        o_ref[u] = (base[u * m:(u + 1) * m] + mm(mm(left[u], blocks), right[u])).astype(BF16)

    def settle(ref, sem):
        pltpu.make_async_copy(ref, ref, sem).wait()

    for g in range(final + 1):
        sent = 3 if g == final and len(late) == 2 else 1 if g == final else 1 + len(flips(g))
        settle(d_in.at[g, :sent], d_send.at[g])
    for k in range(levels + 1):
        @pl.when(owner(k + 1) if k < levels else ones(levels))
        def _(k=k):
            for g in range(final + 1):
                units = 0
                for kind, h in place:
                    if kind != SIB and g == top[h] and k == h - 1 or g < top[h] and k >= groups[g][1]:
                        units += len(targets(kind, h, g))
                if units:
                    settle(base.at[:units * (r * r // m)], w_send.at[g])


def shards(levels, columns, dense_a, dense_b, inner, outer, ascent, descent, couplings):
    r = ascent.shape[-1]
    m = dense_a.shape[-1]
    arrays = (dense_a, dense_b, inner, outer, ascent, descent, couplings)
    vmem = pltpu.VMEM
    dma = pltpu.SemaphoreType.DMA
    groups = split(levels)
    n = len(groups)
    wide = groups[-1][1] - groups[-1][0]
    return pl.pallas_call(
        functools.partial(tree_kernel, levels, columns),
        out_shape=jax.ShapeDtypeStruct(dense_a.shape, BF16),
        in_specs=[pl.BlockSpec(memory_space=pltpu.HBM)] * 7,
        out_specs=pl.BlockSpec(memory_space=pltpu.VMEM),
        scratch_shapes=[
            vmem(dense_a.shape, BF16),
            vmem(dense_b.shape, BF16),
            vmem(inner.shape, BF16),
            vmem(outer.shape, BF16),
            vmem(ascent.shape[1:], BF16),
            vmem(descent.shape[1:], BF16),
            vmem(couplings.shape[1:], BF16),
            vmem((2 * m, m), F32),
            vmem((2, m, wide * r), BF16),
            vmem((2, wide * r, m), BF16),
            vmem((len(kept(levels)), 2, r, r), BF16),
            vmem((n, r, r), BF16),
            vmem((n, r, r), BF16),
            vmem((n, 4, r, r), BF16),
            dma((7,)),
            dma((n,)),
            dma((len(kept(levels)),)),
            dma((n,)),
            dma((2 * n - 1,)),
        ],
        compiler_params=pltpu.CompilerParams(collective_id=0, has_side_effects=True, vmem_limit_bytes=24 * 2**20),
    )(*(pltpu.with_memory_space_constraint(x, pltpu.HBM) for x in arrays))


def solution(mesh):
    rows_, columns = mesh.shape["row"], mesh.shape["col"]
    levels = (rows_ * columns).bit_length() - 1
    both = ("row", "col")
    placed = (
        P(both, None, None),
        P(both, None, None),
        P(both, None, None, None),
        P(both, None, None, None),
        P(both, None, None, None, None),
        P(both, None, None, None, None),
        P(both, None, None, None, None),
    )
    return jax.shard_map(
        functools.partial(shards, levels, columns),
        mesh=mesh, in_specs=placed, out_specs=P(both, None, None), check_vma=False,
    )
```

```python
import functools

import jax
import jax.numpy as jnp
from jax import lax
from jax.experimental import pallas as pl
from jax.experimental.pallas import tpu as pltpu
from jax.sharding import PartitionSpec as P

MESH = pl.DeviceIdType.MESH
BF16 = jnp.bfloat16
F32 = jnp.float32
ASC, DESC, COUP, SIB = 0, 1, 2, 3


def mm(a, b, ca=1, cb=0):
    return lax.dot_general(
        a.astype(BF16), b.astype(BF16), (((ca,), (cb,)), ((), ())), preferred_element_type=F32
    )


def rows(values):
    return jnp.concatenate([v.astype(BF16) for v in values], 0)


def cols(values):
    return jnp.concatenate([v.astype(BF16) for v in values], 1)


def split(levels):
    cuts = [0, *range(1, levels + 1, 2)]
    return list(zip(cuts[:-1], cuts[1:]))


def kept(levels):
    groups = split(levels)
    firsts = [lo + 1 for lo, _ in groups[1:-1]]
    found = [(COUP, h) for h in range(1, levels + 1)]
    found += [(kind, h) for h in range(1, levels - 1) for kind in (ASC, DESC)]
    return found + [(SIB, h) for h in firsts]


def tree_kernel(
    levels, columns,
    da_ref, db_ref, inner_ref, outer_ref, asc_ref, desc_ref, coup_ref, o_ref,
    da, db, inner, outer, asc, desc, coup, base,
    table, t_out, n_out, d_in, cross, near,
    load_sem, w_send, w_recv, d_send, d_recv, c_recv,
):
    pos = lax.axis_index("row") * columns + lax.axis_index("col")
    bit = [pos // 2**i % 2 for i in range(levels)]
    groups = split(levels)
    final = len(groups) - 1
    top = {h: g for g, (lo, hi) in enumerate(groups) for h in range(lo + 1, hi + 1)}
    late = list(range(groups[final][0] + 1, levels + 1))
    r, m = asc.shape[-1], da.shape[-1]
    place = {item: n for n, item in enumerate(kept(levels))}

    def neighbour(g, f, core=0):
        lo, hi = groups[g]
        other = pos + core * (1 - 2 * bit[0])
        for i in range(lo, hi):
            if f >> (i - lo) & 1:
                other = other + 2**i * (1 - 2 * bit[i])
        return other // columns, other % columns

    def flips(g):
        lo, hi = groups[g]
        return list(reversed(range(1, 2 ** (hi - lo))))

    def ones(n):
        return pos % 2**n == 2**n - 1

    def owner(h):
        return pos % 2**h == 2 ** (h - 1) - 1

    barrier = pltpu.get_barrier_semaphore()
    hub, side = ones(1), jnp.logical_not(ones(1))
    mate = neighbour(0, 1)
    greeted = [mate, neighbour(final, 3, 1)]
    peers = [neighbour(g, f) for g in range(1, final + 1) for f in flips(g)]

    def greet(others):
        for other in others:
            pl.semaphore_signal(barrier, inc=1, device_id=other, device_id_type=MESH)

    greet(greeted)
    pl.when(hub)(lambda: greet(peers))

    loads = [
        pltpu.make_async_copy(src, dst, load_sem.at[n])
        for n, (src, dst) in enumerate([
            (asc_ref.at[0], asc),
            (inner_ref, inner),
            (coup_ref.at[0], coup),
            (desc_ref.at[0], desc),
            (da_ref, da),
            (db_ref, db),
            (outer_ref, outer),
        ])
    ]
    for copy in loads[:4]:
        copy.start()

    def slot(kind, h):
        return table.at[place[kind, h]]

    def weight(kind, h, n):
        return table[place[kind, h], n]

    def targets(kind, h, g):
        lo, _ = groups[g]
        if g < top[h]:
            return [(f, kind, slot(kind, h)) for f in flips(g)]
        found = []
        for f in flips(g):
            beyond = f >> (h - lo)
            if kind == ASC:
                found.append((f, SIB if beyond else ASC, slot(ASC, h)))
            elif beyond:
                continue
            elif kind == COUP and f >> (h - 1 - lo) & 1:
                found.append((f, COUP, coup.at[1, 1:3]))
            else:
                found.append((f, kind, slot(kind, h)))
        return found

    def copies(kind, h, g):
        return [
            pltpu.make_async_remote_copy(
                src_ref=src, dst_ref=slot(to, h),
                send_sem=w_send.at[g], recv_sem=w_recv.at[place[to, h]],
                device_id=neighbour(g, f), device_id_type=MESH,
            )
            for f, to, src in targets(kind, h, g)
        ]

    def give(kind, h, gs):
        @pl.when(owner(h))
        def _():
            for g in gs:
                for copy in copies(kind, h, g):
                    copy.start()

    def down(kind, h):
        return list(reversed(range(int(kind in (ASC, SIB) and h > 1), top[h] + 1)))

    def take(kind, h, who=None):
        waits = jnp.logical_not(owner(h)) if kind != SIB else None
        if who is not None:
            waits = who if waits is None else waits & who

        def body():
            pltpu.make_async_copy(slot(kind, h), slot(kind, h), w_recv.at[place[kind, h]]).wait()
            for g in [g for g in down(kind, h) if g < top[h]]:
                @pl.when(ones(groups[g][1]))
                def _(g=g):
                    for copy in copies(kind, h, g):
                        copy.start()

        if waits is None:
            body()
        else:
            pl.when(waits)(body)

    def remote(g, src, dst, recv, to):
        return pltpu.make_async_remote_copy(
            src_ref=src, dst_ref=dst, send_sem=d_send.at[g], recv_sem=recv,
            device_id=to, device_id_type=MESH,
        )

    def send_term(g, f):
        remote(g, t_out.at[g], d_in.at[g, f], d_recv.at[g, f], neighbour(g, f)).start()

    def send_value(g):
        h = groups[g][0] + 1
        remote(g, n_out.at[g], cross.at[h], c_recv.at[h], neighbour(g, 1)).start()

    def landed(ref, sem):
        pltpu.make_async_copy(ref, ref, sem).wait()

    def term_in(g, f):
        landed(d_in.at[g, f], d_recv.at[g, f])

    def value_in(h):
        landed(cross.at[h], c_recv.at[h])

    def pass_value(h):
        remote(top[h], cross.at[h], cross.at[h], c_recv.at[h], mate).start()

    def pass_term(g, f):
        remote(g, d_in.at[g, f], d_in.at[g, f], d_recv.at[g, f], mate).start()

    central = ones(groups[final][0])
    ends = bit[levels - 1] == bit[levels - 2]

    loads[0].wait()
    loads[1].wait()
    for copy in loads[4:]:
        copy.start()
    turned = cols([asc[u, 0].T for u in range(2)])
    lifted_left = mm(asc[2, 0].T, turned).astype(BF16)
    lifted_right = mm(rows([asc[u, 1] for u in range(2)]), asc[2, 1])
    factors = [cols([asc[u, 1], lifted_right[u * r:(u + 1) * r]]) for u in range(2)]
    leaf = [mm(inner[u, 0], inner[u, 1], 0, 0).astype(BF16) for u in range(2)]
    half = rows([mm(leaf[u], factors[u]) for u in range(2)])
    t_out[0] = mm(lifted_left, half[:, r:]).astype(BF16)
    n_out[0] = mm(turned, half[:, :r]).astype(BF16)

    loads[2].wait()
    loads[3].wait()
    for h in range(1, levels + 1):
        @pl.when(owner(h))
        def _(h=h):
            table[place[COUP, h], 0] = coup[1, 0]
            table[place[COUP, h], 1] = coup[1, 3]
            if h < levels - 1:
                table[place[ASC, h], 0] = asc[3, 0].T
                table[place[ASC, h], 1] = asc[3, 1]
                table[place[DESC, h]] = desc[3]

    pl.semaphore_wait(barrier, len(greeted) + len(peers) * bit[0])
    pl.when(side)(lambda: send_term(0, 1))
    send_value(0)
    for h in range(1, levels - 1):
        give(ASC, h, down(ASC, h))
    for h in reversed(late):
        give(COUP, h, [final])

    near[0] = mm(mm(coup[0, 0], leaf[1]), coup[0, 3])
    near[1] = mm(mm(coup[0, 1], leaf[0]), coup[0, 2])
    left_chain = rows([desc[u, 0] for u in range(2)])
    right_chain = rows([desc[u, 1] for u in range(2)])

    def dense():
        loads[4].wait()
        loads[5].wait()
        for u in range(2):
            base[u * m:(u + 1) * m] = mm(da[u], db[u])

    def factors(h, left_chain, right_chain):
        before = mm(left_chain, weight(COUP, h, 0)).astype(BF16)
        return before, mm(weight(COUP, h, 1), right_chain, 1, 1).astype(BF16)

    def couple(value, before, after):
        spread = mm(value, after).astype(BF16)
        for u in range(2):
            near[u] += mm(before[u * r:(u + 1) * r], spread[:, u * r:(u + 1) * r])

    def factors(h, left_chain, right_chain):
        before = mm(left_chain, weight(COUP, h, 0)).astype(BF16)
        return before, mm(weight(COUP, h, 1), right_chain, 1, 1).astype(BF16)

    def couple(value, before, after):
        spread = mm(value, after).astype(BF16)
        for u in range(2):
            near[u] += mm(before[u * r:(u + 1) * r], spread[:, u * r:(u + 1) * r])

    @pl.when(hub)
    def _():
        term_in(0, 1)
        node = (t_out[0].astype(F32) + d_in[0, 1].astype(F32)).astype(BF16)
        n_out[1] = node
        take(ASC, 1)
        t_out[1] = mm(weight(ASC, 1, 0), mm(node, weight(ASC, 1, 1))).astype(BF16)
        for f in flips(1):
            send_term(1, f)

    give(COUP, 1, [0])
    give(DESC, 1, [0])
    loads[4].wait()
    loads[5].wait()
    for u in range(2):
        base[u * m:(u + 1) * m] = mm(da[u], db[u])
    pl.when(hub)(lambda: send_value(1))
    for h in range(2, levels - 1):
        give(COUP, h, down(COUP, h))
        give(DESC, h, down(DESC, h))
    for h in late:
        give(COUP, h, down(COUP, h)[1:])

    @pl.when(hub)
    def _():
        for h in range(2, levels - 1):
            take(ASC, h)
            if (SIB, h) in place:
                take(SIB, h)
        for h in late:
            take(COUP, h, central)

    value_in(1)
    take(COUP, 1)
    take(DESC, 1)
    couple(cross[1], *factors(1, left_chain, right_chain))
    left_chain = mm(left_chain, desc[2, 0]).astype(BF16)
    right_chain = mm(right_chain, desc[2, 1]).astype(BF16)

    @pl.when(hub)
    def _():
        for g in range(1, final):
            lo, hi = groups[g]
            up_left = cols([weight(ASC, lo + 1, 0), weight(SIB, lo + 1, 0)])
            up_right = [weight(ASC, lo + 1, 1), weight(SIB, lo + 1, 1)]
            far_left = mm(weight(ASC, hi, 0), up_left).astype(BF16)
            far_right = mm(rows(up_right), weight(ASC, hi, 1))
            both = [cols([far_right[b * r:(b + 1) * r], up_right[b]]) for b in range(2)]
            for f in (1, 2, 3):
                term_in(g, f)
            own = (t_out[g].astype(F32) + d_in[g, 1].astype(F32)).astype(BF16)
            other = (d_in[g, 2].astype(F32) + d_in[g, 3].astype(F32)).astype(BF16)
            half = rows([mm(own, both[0]), mm(other, both[1])])
            t_out[g + 1] = mm(far_left, half[:, :r]).astype(BF16)
            send_term(g + 1, 3)
            send_term(g + 1, 2)
            if g + 1 < final:
                send_term(g + 1, 1)
            else:
                @pl.when(ends)
                def _():
                    remote(
                        final, t_out.at[final], d_in.at[final, 3], d_recv.at[final, 3],
                        neighbour(final, 3, 1),
                    ).start()
            n_out[g + 1] = mm(up_left, half[:, r:]).astype(BF16)
            send_value(g + 1)
            cross[lo + 2] = other
            pass_value(lo + 2)
            value_in(lo + 1)
            pass_value(lo + 1)

    for h in range(2, late[0]):
        take(COUP, h)
        if h > 2:
            if h > 3:
                take(DESC, h - 2)
            left_chain = mm(left_chain, weight(DESC, h - 2, 0)).astype(BF16)
            right_chain = mm(right_chain, weight(DESC, h - 2, 1)).astype(BF16)
        pl.when(side)(functools.partial(value_in, h))
        couple(cross[h], *factors(h, left_chain, right_chain))
    loads[6].wait()
    for h in late:
        take(DESC, h - 2)
    for h in late:
        take(COUP, h, jnp.logical_not(central))
    before, after = {}, {}
    for h in late:
        left_chain = mm(left_chain, weight(DESC, h - 2, 0)).astype(BF16)
        right_chain = mm(right_chain, weight(DESC, h - 2, 1)).astype(BF16)
        before[h], after[h] = factors(h, left_chain, right_chain)
    before = cols([before[h] for h in late])

    @pl.when(hub)
    def _():
        value_in(late[0])
        pass_value(late[0])
        term_in(final, 2)
        pass_term(final, 2)
        term_in(final, 3)
        pl.when(jnp.logical_not(ends))(lambda: pass_term(final, 3))

    @pl.when(side)
    def _():
        value_in(late[0])
        term_in(final, 2)
        term_in(final, 3)

    last = d_in[final, 2].astype(F32) + d_in[final, 3].astype(F32)
    spread = rows([mm(cross[late[0]], after[late[0]]), mm(last, after[late[1]])])
    for u in range(2):
        value = near[u] + mm(before[u * r:(u + 1) * r], spread[:, u * r:(u + 1) * r])
        o_ref[u] = (base[u * m:(u + 1) * m] + mm(mm(outer[u, 0], value), outer[u, 1], 1, 1)).astype(BF16)

    pl.when(side)(lambda: landed(table.at[0], d_send.at[0]))

    @pl.when(hub)
    def _():
        landed(table.at[0, 0], d_send.at[0])
        for g in range(1, final + 1):
            landed(table.at[:3], d_send.at[g])

    for k in range(levels + 1):
        @pl.when(owner(k + 1) if k < levels else ones(levels))
        def _(k=k):
            for g in range(final + 1):
                units = 0
                for kind, h in place:
                    if g not in down(kind, h):
                        continue
                    if kind != SIB and g == top[h] and k == h - 1 or g < top[h] and k >= groups[g][1]:
                        units += len(targets(kind, h, g))
                if units:
                    landed(base.at[:units * (r * r // m)], w_send.at[g])


def shards(levels, columns, dense_a, dense_b, inner, outer, ascent, descent, couplings):
    r = ascent.shape[-1]
    m = dense_a.shape[-1]
    arrays = (dense_a, dense_b, inner, outer, ascent, descent, couplings)
    vmem = pltpu.VMEM
    dma = pltpu.SemaphoreType.DMA
    groups = split(levels)
    n = len(groups)
    return pl.pallas_call(
        functools.partial(tree_kernel, levels, columns),
        out_shape=jax.ShapeDtypeStruct(dense_a.shape, BF16),
        in_specs=[pl.BlockSpec(memory_space=pltpu.HBM)] * 7,
        out_specs=pl.BlockSpec(memory_space=pltpu.VMEM),
        scratch_shapes=[
            vmem(dense_a.shape, BF16),
            vmem(dense_b.shape, BF16),
            vmem(inner.shape, BF16),
            vmem(outer.shape, BF16),
            vmem(ascent.shape[1:], BF16),
            vmem(descent.shape[1:], BF16),
            vmem(couplings.shape[1:], BF16),
            vmem((2 * m, m), F32),
            vmem((len(kept(levels)), 2, r, r), BF16),
            vmem((n, r, r), BF16),
            vmem((n, r, r), BF16),
            vmem((n, 4, r, r), BF16),
            vmem((levels, r, r), BF16),
            vmem((2, r, r), F32),
            dma((7,)),
            dma((n,)),
            dma((len(kept(levels)),)),
            dma((n,)),
            dma((n, 4)),
            dma((levels,)),
        ],
        compiler_params=pltpu.CompilerParams(collective_id=0, has_side_effects=True, vmem_limit_bytes=24 * 2**20),
    )(*(pltpu.with_memory_space_constraint(x, pltpu.HBM) for x in arrays))


def solution(mesh):
    rows_, columns = mesh.shape["row"], mesh.shape["col"]
    levels = (rows_ * columns).bit_length() - 1
    both = ("row", "col")
    placed = (
        P(both, None, None),
        P(both, None, None),
        P(both, None, None, None),
        P(both, None, None, None),
        P(both, None, None, None, None),
        P(both, None, None, None, None),
        P(both, None, None, None, None),
    )
    return jax.shard_map(
        functools.partial(shards, levels, columns),
        mesh=mesh, in_specs=placed, out_specs=P(both, None, None), check_vma=False,
    )
```

```python
import functools

import jax
import jax.numpy as jnp
from jax import lax
from jax.experimental import pallas as pl
from jax.experimental.pallas import tpu as pltpu
from jax.sharding import PartitionSpec as P

MESH = pl.DeviceIdType.MESH
BF16 = jnp.bfloat16
F32 = jnp.float32
ASC, DESC, COUP, SIB = 0, 1, 2, 3


def mm(a, b, ca=1, cb=0):
    return lax.dot_general(
        a.astype(BF16), b.astype(BF16), (((ca,), (cb,)), ((), ())), preferred_element_type=F32
    )


def rows(values):
    return jnp.concatenate([v.astype(BF16) for v in values], 0)


def cols(values):
    return jnp.concatenate([v.astype(BF16) for v in values], 1)


def split(levels):
    cuts = [0, *range(1, levels + 1, 2)]
    return list(zip(cuts[:-1], cuts[1:]))


def kept(levels):
    groups = split(levels)
    firsts = [lo + 1 for lo, _ in groups[1:-1]]
    found = [(COUP, h) for h in range(1, levels + 1)]
    found += [(kind, h) for h in range(1, levels - 1) for kind in (ASC, DESC)]
    return found + [(SIB, h) for h in firsts]


def tree_kernel(
    levels, columns,
    da_ref, db_ref, inner_ref, outer_ref, asc_ref, desc_ref, coup_ref, o_ref,
    da, db, inner, outer, asc, desc, coup, base, left, right,
    table, t_out, n_out, d_in, cross, near,
    load_sem, w_send, w_recv, d_send, d_recv, c_recv,
):
    pos = lax.axis_index("row") * columns + lax.axis_index("col")
    bit = [pos // 2**i % 2 for i in range(levels)]
    groups = split(levels)
    final = len(groups) - 1
    top = {h: g for g, (lo, hi) in enumerate(groups) for h in range(lo + 1, hi + 1)}
    late = list(range(groups[final][0] + 1, levels + 1))
    r, m = asc.shape[-1], da.shape[-1]
    place = {item: n for n, item in enumerate(kept(levels))}

    def neighbour(g, f, core=0):
        lo, hi = groups[g]
        other = pos + core * (1 - 2 * bit[0])
        for i in range(lo, hi):
            if f >> (i - lo) & 1:
                other = other + 2**i * (1 - 2 * bit[i])
        return other // columns, other % columns

    def flips(g):
        lo, hi = groups[g]
        return [f for f in (1, 3, 2) if f < 2 ** (hi - lo)]

    def ones(n):
        return pos % 2**n == 2**n - 1

    def owner(h):
        return pos % 2**h == 2 ** (h - 1) - 1

    barrier = pltpu.get_barrier_semaphore()
    hub, side = ones(1), jnp.logical_not(ones(1))
    mate = neighbour(0, 1)
    greeted = [mate, neighbour(final, 3, 1)]
    peers = [neighbour(g, f) for g in range(1, final + 1) for f in flips(g)]

    def greet(others):
        for other in others:
            pl.semaphore_signal(barrier, inc=1, device_id=other, device_id_type=MESH)

    greet(greeted)
    pl.when(hub)(lambda: greet(peers))

    loads = [
        pltpu.make_async_copy(src, dst, load_sem.at[n])
        for n, (src, dst) in enumerate([
            (asc_ref.at[0], asc),
            (inner_ref, inner),
            (coup_ref.at[0], coup),
            (desc_ref.at[0], desc),
            (da_ref, da),
            (db_ref, db),
            (outer_ref, outer),
        ])
    ]
    for copy in loads[:4]:
        copy.start()

    def slot(kind, h):
        return table.at[place[kind, h]]

    def weight(kind, h, n):
        return table[place[kind, h], n]

    def targets(kind, h, g):
        lo, _ = groups[g]
        if g < top[h]:
            return [(f, kind, slot(kind, h)) for f in flips(g)]
        found = []
        for f in flips(g):
            beyond = f >> (h - lo)
            if kind == ASC:
                found.append((f, SIB if beyond else ASC, slot(ASC, h)))
            elif beyond:
                continue
            elif kind == COUP and f >> (h - 1 - lo) & 1:
                found.append((f, COUP, coup.at[1, 1:3]))
            else:
                found.append((f, kind, slot(kind, h)))
        return found

    def copies(kind, h, g):
        return [
            pltpu.make_async_remote_copy(
                src_ref=src, dst_ref=slot(to, h),
                send_sem=w_send.at[g], recv_sem=w_recv.at[place[to, h]],
                device_id=neighbour(g, f), device_id_type=MESH,
            )
            for f, to, src in targets(kind, h, g)
        ]

    def give(kind, h, gs):
        @pl.when(owner(h))
        def _():
            for g in gs:
                for copy in copies(kind, h, g):
                    copy.start()

    def down(kind, h):
        return list(reversed(range(int(kind in (ASC, SIB) and h > 1), top[h] + 1)))

    def take(kind, h, who=None):
        waits = jnp.logical_not(owner(h)) if kind != SIB else None
        if who is not None:
            waits = who if waits is None else waits & who

        def body():
            pltpu.make_async_copy(slot(kind, h), slot(kind, h), w_recv.at[place[kind, h]]).wait()
            for g in [g for g in down(kind, h) if g < top[h]]:
                @pl.when(ones(groups[g][1]))
                def _(g=g):
                    for copy in copies(kind, h, g):
                        copy.start()

        if waits is None:
            body()
        else:
            pl.when(waits)(body)

    def remote(g, src, dst, recv, to):
        return pltpu.make_async_remote_copy(
            src_ref=src, dst_ref=dst, send_sem=d_send.at[g], recv_sem=recv,
            device_id=to, device_id_type=MESH,
        )

    def send_term(g, f):
        remote(g, t_out.at[g], d_in.at[g, f], d_recv.at[g, f], neighbour(g, f)).start()

    def send_value(g):
        h = groups[g][0] + 1
        remote(g, n_out.at[g], cross.at[h], c_recv.at[h], neighbour(g, 1)).start()

    def landed(ref, sem):
        pltpu.make_async_copy(ref, ref, sem).wait()

    def term_in(g, f):
        landed(d_in.at[g, f], d_recv.at[g, f])

    def value_in(h):
        landed(cross.at[h], c_recv.at[h])

    def pass_value(h):
        remote(top[h], cross.at[h], cross.at[h], c_recv.at[h], mate).start()

    def pass_term(g, f):
        remote(g, d_in.at[g, f], d_in.at[g, f], d_recv.at[g, f], mate).start()

    central = ones(groups[final][0])
    ends = bit[levels - 1] == bit[levels - 2]

    loads[0].wait()
    for h in range(1, levels - 1):
        @pl.when(owner(h))
        def _(h=h):
            table[place[ASC, h], 0] = asc[3, 0].T
            table[place[ASC, h], 1] = asc[3, 1]

    loads[1].wait()
    for copy in loads[4:]:
        copy.start()
    turned = cols([asc[u, 0].T for u in range(2)])
    lifted_left = mm(asc[2, 0].T, turned).astype(BF16)
    lifted_right = mm(rows([asc[u, 1] for u in range(2)]), asc[2, 1])
    factors = [cols([asc[u, 1], lifted_right[u * r:(u + 1) * r]]) for u in range(2)]
    leaf = [mm(inner[u, 0], inner[u, 1], 0, 0).astype(BF16) for u in range(2)]
    half = rows([mm(leaf[u], factors[u]) for u in range(2)])
    t_out[0] = mm(lifted_left, half[:, r:]).astype(BF16)
    n_out[0] = mm(turned, half[:, :r]).astype(BF16)

    pl.semaphore_wait(barrier, len(greeted) + len(peers) * bit[0])
    pl.when(side)(lambda: send_term(0, 1))
    for h in range(1, levels - 1):
        give(ASC, h, down(ASC, h))
    send_value(0)
    loads[2].wait()
    loads[3].wait()
    for h in reversed(range(1, levels + 1)):
        @pl.when(owner(h))
        def _(h=h):
            table[place[COUP, h], 0] = coup[1, 0]
            table[place[COUP, h], 1] = coup[1, 3]
            if h < levels - 1:
                table[place[DESC, h]] = desc[3]

        if h in late:
            give(COUP, h, [final])
        if h == 1:
            give(COUP, 1, [0])
            give(DESC, 1, [0])

    left_chain = rows([desc[u, 0] for u in range(2)])
    right_chain = rows([desc[u, 1] for u in range(2)])

    def dense():
        loads[4].wait()
        loads[5].wait()
        for u in range(2):
            base[u * m:(u + 1) * m] = mm(da[u], db[u])

    def factors(h, left_chain, right_chain):
        before = mm(left_chain, weight(COUP, h, 0)).astype(BF16)
        return before, mm(weight(COUP, h, 1), right_chain, 1, 1).astype(BF16)

    def couple(value, before, after):
        spread = mm(value, after).astype(BF16)
        for u in range(2):
            near[u] += mm(before[u * r:(u + 1) * r], spread[:, u * r:(u + 1) * r])

    def factors(h, left_chain, right_chain):
        before = mm(left_chain, weight(COUP, h, 0)).astype(BF16)
        return before, mm(weight(COUP, h, 1), right_chain, 1, 1).astype(BF16)

    def couple(value, before, after):
        spread = mm(value, after).astype(BF16)
        for u in range(2):
            near[u] += mm(before[u * r:(u + 1) * r], spread[:, u * r:(u + 1) * r])

    @pl.when(hub)
    def _():
        term_in(0, 1)
        node = (t_out[0].astype(F32) + d_in[0, 1].astype(F32)).astype(BF16)
        n_out[1] = node
        take(ASC, 1)
        t_out[1] = mm(weight(ASC, 1, 0), mm(node, weight(ASC, 1, 1))).astype(BF16)
        for f in flips(1):
            send_term(1, f)

    pl.when(hub)(lambda: send_value(1))
    for h in range(2, levels - 1):
        give(COUP, h, down(COUP, h))
        give(DESC, h, down(DESC, h))
    for h in late:
        give(COUP, h, down(COUP, h)[1:])
    loads[4].wait()
    loads[5].wait()
    for u in range(2):
        base[u * m:(u + 1) * m] = mm(da[u], db[u])

    @pl.when(central)
    def _():
        for h in late:
            take(COUP, h)

    near[0] = mm(mm(coup[0, 0], leaf[1]), coup[0, 3])
    near[1] = mm(mm(coup[0, 1], leaf[0]), coup[0, 2])
    value_in(1)
    take(COUP, 1)
    take(DESC, 1)
    couple(cross[1], *factors(1, left_chain, right_chain))
    left_chain = mm(left_chain, desc[2, 0]).astype(BF16)
    right_chain = mm(right_chain, desc[2, 1]).astype(BF16)

    @pl.when(hub)
    def _():
        for h in range(2, levels - 1):
            take(ASC, h)
            if (SIB, h) in place:
                take(SIB, h)

    @pl.when(hub)
    def _():
        for g in range(1, final):
            lo, hi = groups[g]
            up_left = cols([weight(ASC, lo + 1, 0), weight(SIB, lo + 1, 0)])
            up_right = [weight(ASC, lo + 1, 1), weight(SIB, lo + 1, 1)]
            far_left = mm(weight(ASC, hi, 0), up_left).astype(BF16)
            far_right = mm(rows(up_right), weight(ASC, hi, 1))
            both = [cols([far_right[b * r:(b + 1) * r], up_right[b]]) for b in range(2)]
            for f in (1, 2, 3):
                term_in(g, f)
            own = (t_out[g].astype(F32) + d_in[g, 1].astype(F32)).astype(BF16)
            other = (d_in[g, 2].astype(F32) + d_in[g, 3].astype(F32)).astype(BF16)
            half = rows([mm(own, both[0]), mm(other, both[1])])
            t_out[g + 1] = mm(far_left, half[:, :r]).astype(BF16)
            if g + 1 == final:
                @pl.when(ends)
                def _():
                    remote(
                        final, t_out.at[final], d_in.at[final, 3], d_recv.at[final, 3],
                        neighbour(final, 3, 1),
                    ).start()
            send_term(g + 1, 3)
            send_term(g + 1, 2)
            if g + 1 < final:
                send_term(g + 1, 1)
            n_out[g + 1] = mm(up_left, half[:, r:]).astype(BF16)
            send_value(g + 1)
            cross[lo + 2] = other
            pass_value(lo + 2)
            value_in(lo + 1)
            pass_value(lo + 1)

    near_levels = range(2, late[0])
    loads[6].wait()
    ready, chains = {}, {}
    for h in near_levels:
        if h > 2:
            if h > 3:
                take(DESC, h - 2)
            left_chain = mm(left_chain, weight(DESC, h - 2, 0)).astype(BF16)
            right_chain = mm(right_chain, weight(DESC, h - 2, 1)).astype(BF16)
        chains[h] = left_chain, right_chain
        if h < late[0] - 1:
            take(COUP, h)
            ready[h] = factors(h, *chains[h])
    if late[0] > 3:
        take(DESC, late[0] - 2)
    left_chain = mm(left_chain, weight(DESC, late[0] - 2, 0)).astype(BF16)
    right_chain = mm(right_chain, weight(DESC, late[0] - 2, 1)).astype(BF16)
    left_base = [mm(outer[u, 0], left_chain[u * r:(u + 1) * r]).astype(BF16) for u in range(2)]
    right_base = [mm(outer[u, 1], right_chain[u * r:(u + 1) * r]).astype(BF16) for u in range(2)]
    take(COUP, late[0] - 1)
    ready[late[0] - 1] = factors(late[0] - 1, *chains[late[0] - 1])

    @pl.when(side)
    def _():
        for h in near_levels:
            value_in(h)

    for h in near_levels:
        couple(cross[h], *ready[h])
    for u in range(2):
        base[u * m:(u + 1) * m] += mm(mm(outer[u, 0], near[u]), outer[u, 1], 1, 1)
    take(DESC, late[1] - 2)
    for h in late:
        take(COUP, h, jnp.logical_not(central))
    first = cols([weight(COUP, late[0], 0), mm(weight(DESC, late[1] - 2, 0), weight(COUP, late[1], 0))])
    second = rows([
        weight(COUP, late[0], 1),
        mm(weight(COUP, late[1], 1), weight(DESC, late[1] - 2, 1), 1, 1),
    ])
    for u in range(2):
        left[u] = mm(left_base[u], first).astype(BF16)
        right[u] = mm(second, right_base[u], 1, 1).astype(BF16)

    @pl.when(hub)
    def _():
        value_in(late[0])
        pass_value(late[0])
        term_in(final, 2)
        pass_term(final, 2)
        term_in(final, 3)
        pl.when(jnp.logical_not(ends))(lambda: pass_term(final, 3))

    @pl.when(side)
    def _():
        value_in(late[0])
        term_in(final, 2)
        term_in(final, 3)

    last = (d_in[final, 2].astype(F32) + d_in[final, 3].astype(F32)).astype(BF16)
    zero = jnp.zeros_like(last)
    blocks = rows([cols([cross[late[0]], zero]), cols([zero, last])])
    for u in range(2):
        o_ref[u] = (base[u * m:(u + 1) * m] + mm(mm(left[u], blocks), right[u])).astype(BF16)

    pl.when(side)(lambda: landed(table.at[0], d_send.at[0]))

    @pl.when(hub)
    def _():
        landed(table.at[0, 0], d_send.at[0])
        for g in range(1, final + 1):
            landed(table.at[:3], d_send.at[g])

    for k in range(levels + 1):
        @pl.when(owner(k + 1) if k < levels else ones(levels))
        def _(k=k):
            for g in range(final + 1):
                units = 0
                for kind, h in place:
                    if g not in down(kind, h):
                        continue
                    if kind != SIB and g == top[h] and k == h - 1 or g < top[h] and k >= groups[g][1]:
                        units += len(targets(kind, h, g))
                if units:
                    landed(base.at[:units * (r * r // m)], w_send.at[g])


def shards(levels, columns, dense_a, dense_b, inner, outer, ascent, descent, couplings):
    r = ascent.shape[-1]
    m = dense_a.shape[-1]
    arrays = (dense_a, dense_b, inner, outer, ascent, descent, couplings)
    vmem = pltpu.VMEM
    dma = pltpu.SemaphoreType.DMA
    groups = split(levels)
    n = len(groups)
    return pl.pallas_call(
        functools.partial(tree_kernel, levels, columns),
        out_shape=jax.ShapeDtypeStruct(dense_a.shape, BF16),
        in_specs=[pl.BlockSpec(memory_space=pltpu.HBM)] * 7,
        out_specs=pl.BlockSpec(memory_space=pltpu.VMEM),
        scratch_shapes=[
            vmem(dense_a.shape, BF16),
            vmem(dense_b.shape, BF16),
            vmem(inner.shape, BF16),
            vmem(outer.shape, BF16),
            vmem(ascent.shape[1:], BF16),
            vmem(descent.shape[1:], BF16),
            vmem(couplings.shape[1:], BF16),
            vmem((2 * m, m), F32),
            vmem((2, m, 2 * r), BF16),
            vmem((2, 2 * r, m), BF16),
            vmem((len(kept(levels)), 2, r, r), BF16),
            vmem((n, r, r), BF16),
            vmem((n, r, r), BF16),
            vmem((n, 4, r, r), BF16),
            vmem((levels, r, r), BF16),
            vmem((2, r, r), F32),
            dma((7,)),
            dma((n,)),
            dma((len(kept(levels)),)),
            dma((n,)),
            dma((n, 4)),
            dma((levels,)),
        ],
        compiler_params=pltpu.CompilerParams(collective_id=0, has_side_effects=True, vmem_limit_bytes=24 * 2**20),
    )(*(pltpu.with_memory_space_constraint(x, pltpu.HBM) for x in arrays))


def solution(mesh):
    rows_, columns = mesh.shape["row"], mesh.shape["col"]
    levels = (rows_ * columns).bit_length() - 1
    both = ("row", "col")
    placed = (
        P(both, None, None),
        P(both, None, None),
        P(both, None, None, None),
        P(both, None, None, None),
        P(both, None, None, None, None),
        P(both, None, None, None, None),
        P(both, None, None, None, None),
    )
    return jax.shard_map(
        functools.partial(shards, levels, columns),
        mesh=mesh, in_specs=placed, out_specs=P(both, None, None), check_vma=False,
    )
```

```python
import functools

import jax
import jax.numpy as jnp
from jax import lax
from jax.experimental import pallas as pl
from jax.experimental.pallas import tpu as pltpu
from jax.sharding import PartitionSpec as P

MESH = pl.DeviceIdType.MESH
BF16 = jnp.bfloat16
F32 = jnp.float32
ASC, DESC, COUP, SIB = 0, 1, 2, 3


def mm(a, b, ca=1, cb=0):
    return lax.dot_general(
        a.astype(BF16), b.astype(BF16), (((ca,), (cb,)), ((), ())), preferred_element_type=F32
    )


def rows(values):
    return jnp.concatenate([v.astype(BF16) for v in values], 0)


def cols(values):
    return jnp.concatenate([v.astype(BF16) for v in values], 1)


def split(levels):
    cuts = [0, *range(1, levels + 1, 2)]
    return list(zip(cuts[:-1], cuts[1:]))


def kept(levels):
    groups = split(levels)
    firsts = [lo + 1 for lo, _ in groups[1:-1]]
    found = [(COUP, h) for h in range(1, levels + 1)]
    found += [(kind, h) for h in range(1, levels - 1) for kind in (ASC, DESC)]
    return found + [(SIB, h) for h in firsts]


def tree_kernel(
    levels, columns,
    da_ref, db_ref, inner_ref, outer_ref, asc_ref, desc_ref, coup_ref, o_ref,
    da, db, inner, outer, asc, desc, coup, base, left, right,
    table, t_out, n_out, d_in, cross, near,
    load_sem, w_send, w_recv, d_send, d_recv, c_recv, told_sem,
):
    pos = lax.axis_index("row") * columns + lax.axis_index("col")
    bit = [pos // 2**i % 2 for i in range(levels)]
    groups = split(levels)
    final = len(groups) - 1
    top = {h: g for g, (lo, hi) in enumerate(groups) for h in range(lo + 1, hi + 1)}
    late = list(range(groups[final][0] + 1, levels + 1))
    r, m = asc.shape[-1], da.shape[-1]
    place = {item: n for n, item in enumerate(kept(levels))}

    def neighbour(g, f, core=0):
        lo, hi = groups[g]
        other = pos + core * (1 - 2 * bit[0])
        for i in range(lo, hi):
            if f >> (i - lo) & 1:
                other = other + 2**i * (1 - 2 * bit[i])
        return other // columns, other % columns

    def flips(g):
        lo, hi = groups[g]
        return [f for f in (1, 3, 2) if f < 2 ** (hi - lo)]

    def ones(n):
        return pos % 2**n == 2**n - 1

    def owner(h):
        return pos % 2**h == 2 ** (h - 1) - 1

    barrier = pltpu.get_barrier_semaphore()
    hub, side = ones(1), jnp.logical_not(ones(1))
    mate = neighbour(0, 1)
    lower = [neighbour(g, f) for g in range(1, final) for f in flips(g)]
    upper = [neighbour(final, f, 1) for f in flips(final)]

    def greet(others):
        for other in others:
            pl.semaphore_signal(barrier, inc=1, device_id=other, device_id_type=MESH)

    greet([mate])

    @pl.when(hub)
    def _():
        greet(lower)
        greet(upper)

    pl.when(side)(lambda: greet([neighbour(final, f) for f in flips(final)]))

    loads = [
        pltpu.make_async_copy(src, dst, load_sem.at[n])
        for n, (src, dst) in enumerate([
            (asc_ref.at[0], asc),
            (inner_ref, inner),
            (coup_ref.at[0], coup),
            (desc_ref.at[0], desc),
            (da_ref, da),
            (db_ref, db),
            (outer_ref, outer),
        ])
    ]
    for copy in loads[:4]:
        copy.start()

    def slot(kind, h):
        return table.at[place[kind, h]]

    def weight(kind, h, n):
        return table[place[kind, h], n]

    def targets(kind, h, g):
        lo, _ = groups[g]
        if g < top[h]:
            return [(f, kind, slot(kind, h)) for f in flips(g)]
        found = []
        for f in flips(g):
            beyond = f >> (h - lo)
            if kind == ASC:
                found.append((f, SIB if beyond else ASC, slot(ASC, h)))
            elif beyond:
                continue
            elif kind == COUP and f >> (h - 1 - lo) & 1:
                found.append((f, COUP, coup.at[1, 1:3]))
            else:
                found.append((f, kind, slot(kind, h)))
        return found

    def copies(kind, h, g):
        return [
            pltpu.make_async_remote_copy(
                src_ref=src, dst_ref=slot(to, h),
                send_sem=w_send.at[g], recv_sem=w_recv.at[place[to, h]],
                device_id=neighbour(g, f), device_id_type=MESH,
            )
            for f, to, src in targets(kind, h, g)
        ]

    def give(kind, h, gs):
        @pl.when(owner(h))
        def _():
            for g in gs:
                for copy in copies(kind, h, g):
                    copy.start()

    def down(kind, h):
        return list(reversed(range(int(kind in (ASC, SIB) and h > 1), top[h] + 1)))

    def take(kind, h, who=None):
        waits = jnp.logical_not(owner(h)) if kind != SIB else None
        if who is not None:
            waits = who if waits is None else waits & who

        def body():
            pltpu.make_async_copy(slot(kind, h), slot(kind, h), w_recv.at[place[kind, h]]).wait()
            for g in [g for g in down(kind, h) if g < top[h]]:
                @pl.when(ones(groups[g][1]))
                def _(g=g):
                    for copy in copies(kind, h, g):
                        copy.start()

        if waits is None:
            body()
        else:
            pl.when(waits)(body)

    def remote(g, src, dst, recv, to):
        return pltpu.make_async_remote_copy(
            src_ref=src, dst_ref=dst, send_sem=d_send.at[g], recv_sem=recv,
            device_id=to, device_id_type=MESH,
        )

    def send_term(g, f, core=0):
        remote(g, t_out.at[g], d_in.at[g, f], d_recv.at[g, f], neighbour(g, f, core)).start()

    def send_value(g, core=0):
        h = groups[g][0] + 1
        remote(g, n_out.at[g], cross.at[h], c_recv.at[h], neighbour(g, 1, core)).start()

    def landed(ref, sem):
        pltpu.make_async_copy(ref, ref, sem).wait()

    def term_in(g, f):
        landed(d_in.at[g, f], d_recv.at[g, f])

    def value_in(h):
        landed(cross.at[h], c_recv.at[h])

    def pass_value(h):
        remote(top[h], cross.at[h], cross.at[h], c_recv.at[h], mate).start()

    def pass_term(g, f):
        remote(g, d_in.at[g, f], d_in.at[g, f], d_recv.at[g, f], mate).start()

    central = ones(groups[final][0])
    ends = bit[levels - 1] == bit[levels - 2]

    loads[0].wait()
    for h in range(1, levels - 1):
        @pl.when(owner(h))
        def _(h=h):
            table[place[ASC, h], 0] = asc[3, 0].T
            table[place[ASC, h], 1] = asc[3, 1]

    loads[1].wait()
    for copy in loads[4:]:
        copy.start()
    turned = cols([asc[u, 0].T for u in range(2)])
    lifted_left = mm(asc[2, 0].T, turned).astype(BF16)
    lifted_right = mm(rows([asc[u, 1] for u in range(2)]), asc[2, 1])
    factors = [cols([asc[u, 1], lifted_right[u * r:(u + 1) * r]]) for u in range(2)]
    leaf = [mm(inner[u, 0], inner[u, 1], 0, 0).astype(BF16) for u in range(2)]
    half = rows([mm(leaf[u], factors[u]) for u in range(2)])
    t_out[0] = mm(lifted_left, half[:, r:]).astype(BF16)
    n_out[0] = mm(turned, half[:, :r]).astype(BF16)

    def tell_mate():
        pl.semaphore_signal(told_sem, inc=1, device_id=mate, device_id_type=MESH)

    @pl.when(hub)
    def _():
        pl.semaphore_wait(barrier, 1 + len(lower))
        tell_mate()

    @pl.when(side)
    def _():
        pl.semaphore_wait(told_sem, 1)
        send_term(0, 1)

    for h in range(1, levels - 1):
        give(ASC, h, down(ASC, h))
    send_value(0)
    loads[2].wait()
    loads[3].wait()
    for h in reversed(range(1, levels + 1)):
        @pl.when(owner(h))
        def _(h=h):
            table[place[COUP, h], 0] = coup[1, 0]
            table[place[COUP, h], 1] = coup[1, 3]
            if h < levels - 1:
                table[place[DESC, h]] = desc[3]

        if h == 1:
            give(COUP, 1, [0])
            give(DESC, 1, [0])

    @pl.when(side)
    def _():
        pl.semaphore_wait(barrier, 1 + 2 * len(upper))
        tell_mate()

    left_chain = rows([desc[u, 0] for u in range(2)])
    right_chain = rows([desc[u, 1] for u in range(2)])

    def factors(h, left_chain, right_chain):
        before = mm(left_chain, weight(COUP, h, 0)).astype(BF16)
        return before, mm(weight(COUP, h, 1), right_chain, 1, 1).astype(BF16)

    def couple(value, before, after):
        spread = mm(value, after).astype(BF16)
        for u in range(2):
            near[u] += mm(before[u * r:(u + 1) * r], spread[:, u * r:(u + 1) * r])

    @pl.when(hub)
    def _():
        term_in(0, 1)
        node = (t_out[0].astype(F32) + d_in[0, 1].astype(F32)).astype(BF16)
        n_out[1] = node
        take(ASC, 1)
        t_out[1] = mm(weight(ASC, 1, 0), mm(node, weight(ASC, 1, 1))).astype(BF16)
        for f in flips(1):
            send_term(1, f)

    gives_top = owner(late[0]) | owner(late[1])

    @pl.when(gives_top)
    def _():
        pl.semaphore_wait(told_sem, 1)
        for h in reversed(late):
            give(COUP, h, [final])

    pl.when(hub)(lambda: send_value(1))
    for h in range(2, levels - 1):
        give(COUP, h, down(COUP, h))
        give(DESC, h, down(DESC, h))
    for h in late:
        give(COUP, h, down(COUP, h)[1:])
    loads[4].wait()
    loads[5].wait()
    for u in range(2):
        base[u * m:(u + 1) * m] = mm(da[u], db[u])

    @pl.when(central)
    def _():
        for h in late:
            take(COUP, h)

    near[0] = mm(mm(coup[0, 0], leaf[1]), coup[0, 3])
    near[1] = mm(mm(coup[0, 1], leaf[0]), coup[0, 2])
    value_in(1)
    take(COUP, 1)
    take(DESC, 1)
    couple(cross[1], *factors(1, left_chain, right_chain))
    left_chain = mm(left_chain, desc[2, 0]).astype(BF16)
    right_chain = mm(right_chain, desc[2, 1]).astype(BF16)

    @pl.when(hub)
    def _():
        for h in range(2, levels - 1):
            take(ASC, h)
            if (SIB, h) in place:
                take(SIB, h)

    @pl.when(hub)
    def _():
        for g in range(1, final):
            lo, hi = groups[g]
            up_left = cols([weight(ASC, lo + 1, 0), weight(SIB, lo + 1, 0)])
            up_right = [weight(ASC, lo + 1, 1), weight(SIB, lo + 1, 1)]
            far_left = mm(weight(ASC, hi, 0), up_left).astype(BF16)
            far_right = mm(rows(up_right), weight(ASC, hi, 1))
            both = [cols([far_right[b * r:(b + 1) * r], up_right[b]]) for b in range(2)]
            for f in (1, 2, 3):
                term_in(g, f)
            own = (t_out[g].astype(F32) + d_in[g, 1].astype(F32)).astype(BF16)
            other = (d_in[g, 2].astype(F32) + d_in[g, 3].astype(F32)).astype(BF16)
            half = rows([mm(own, both[0]), mm(other, both[1])])
            t_out[g + 1] = mm(far_left, half[:, :r]).astype(BF16)
            if g + 1 == final:
                pl.when(jnp.logical_not(gives_top))(lambda: pl.semaphore_wait(told_sem, 1))
                pl.when(ends)(lambda: send_term(final, 3, 1))
                send_term(final, 3)
                send_term(final, 2)
                send_term(final, 2, 1)
            else:
                for f in flips(g + 1):
                    send_term(g + 1, f)
            n_out[g + 1] = mm(up_left, half[:, r:]).astype(BF16)
            send_value(g + 1)
            if g + 1 == final:
                send_value(final, 1)
            cross[lo + 2] = other
            pass_value(lo + 2)
            value_in(lo + 1)
            pass_value(lo + 1)

    near_levels = range(2, late[0])
    loads[6].wait()
    ready, chains = {}, {}
    for h in near_levels:
        if h > 2:
            if h > 3:
                take(DESC, h - 2)
            left_chain = mm(left_chain, weight(DESC, h - 2, 0)).astype(BF16)
            right_chain = mm(right_chain, weight(DESC, h - 2, 1)).astype(BF16)
        chains[h] = left_chain, right_chain
        if h < late[0] - 1:
            take(COUP, h)
            ready[h] = factors(h, *chains[h])
    if late[0] > 3:
        take(DESC, late[0] - 2)
    left_chain = mm(left_chain, weight(DESC, late[0] - 2, 0)).astype(BF16)
    right_chain = mm(right_chain, weight(DESC, late[0] - 2, 1)).astype(BF16)
    left_base = [mm(outer[u, 0], left_chain[u * r:(u + 1) * r]).astype(BF16) for u in range(2)]
    right_base = [mm(outer[u, 1], right_chain[u * r:(u + 1) * r]).astype(BF16) for u in range(2)]
    take(COUP, late[0] - 1)
    ready[late[0] - 1] = factors(late[0] - 1, *chains[late[0] - 1])

    @pl.when(side)
    def _():
        for h in near_levels:
            value_in(h)

    for h in near_levels:
        couple(cross[h], *ready[h])
    for u in range(2):
        base[u * m:(u + 1) * m] += mm(mm(outer[u, 0], near[u]), outer[u, 1], 1, 1)
    take(DESC, late[1] - 2)
    for h in late:
        take(COUP, h, jnp.logical_not(central))
    first = cols([weight(COUP, late[0], 0), mm(weight(DESC, late[1] - 2, 0), weight(COUP, late[1], 0))])
    second = rows([
        weight(COUP, late[0], 1),
        mm(weight(COUP, late[1], 1), weight(DESC, late[1] - 2, 1), 1, 1),
    ])
    for u in range(2):
        left[u] = mm(left_base[u], first).astype(BF16)
        right[u] = mm(second, right_base[u], 1, 1).astype(BF16)

    value_in(late[0])
    term_in(final, 2)
    term_in(final, 3)
    pl.when(hub & jnp.logical_not(ends))(lambda: pass_term(final, 3))

    last = (d_in[final, 2].astype(F32) + d_in[final, 3].astype(F32)).astype(BF16)
    zero = jnp.zeros_like(last)
    blocks = rows([cols([cross[late[0]], zero]), cols([zero, last])])
    for u in range(2):
        o_ref[u] = (base[u * m:(u + 1) * m] + mm(mm(left[u], blocks), right[u])).astype(BF16)

    pl.when(side)(lambda: landed(table.at[0], d_send.at[0]))

    @pl.when(hub)
    def _():
        landed(table.at[0, 0], d_send.at[0])
        for g in range(1, final + 1):
            landed(table.at[:3], d_send.at[g])

    for k in range(levels + 1):
        @pl.when(owner(k + 1) if k < levels else ones(levels))
        def _(k=k):
            for g in range(final + 1):
                units = 0
                for kind, h in place:
                    if g not in down(kind, h):
                        continue
                    if kind != SIB and g == top[h] and k == h - 1 or g < top[h] and k >= groups[g][1]:
                        units += len(targets(kind, h, g))
                if units:
                    landed(base.at[:units * (r * r // m)], w_send.at[g])


def shards(levels, columns, dense_a, dense_b, inner, outer, ascent, descent, couplings):
    r = ascent.shape[-1]
    m = dense_a.shape[-1]
    arrays = (dense_a, dense_b, inner, outer, ascent, descent, couplings)
    vmem = pltpu.VMEM
    dma = pltpu.SemaphoreType.DMA
    groups = split(levels)
    n = len(groups)
    return pl.pallas_call(
        functools.partial(tree_kernel, levels, columns),
        out_shape=jax.ShapeDtypeStruct(dense_a.shape, BF16),
        in_specs=[pl.BlockSpec(memory_space=pltpu.HBM)] * 7,
        out_specs=pl.BlockSpec(memory_space=pltpu.VMEM),
        scratch_shapes=[
            vmem(dense_a.shape, BF16),
            vmem(dense_b.shape, BF16),
            vmem(inner.shape, BF16),
            vmem(outer.shape, BF16),
            vmem(ascent.shape[1:], BF16),
            vmem(descent.shape[1:], BF16),
            vmem(couplings.shape[1:], BF16),
            vmem((2 * m, m), F32),
            vmem((2, m, 2 * r), BF16),
            vmem((2, 2 * r, m), BF16),
            vmem((len(kept(levels)), 2, r, r), BF16),
            vmem((n, r, r), BF16),
            vmem((n, r, r), BF16),
            vmem((n, 4, r, r), BF16),
            vmem((levels, r, r), BF16),
            vmem((2, r, r), F32),
            dma((7,)),
            dma((n,)),
            dma((len(kept(levels)),)),
            dma((n,)),
            dma((n, 4)),
            dma((levels,)),
            pltpu.SemaphoreType.REGULAR,
        ],
        compiler_params=pltpu.CompilerParams(collective_id=0, has_side_effects=True, vmem_limit_bytes=24 * 2**20),
    )(*(pltpu.with_memory_space_constraint(x, pltpu.HBM) for x in arrays))


def solution(mesh):
    rows_, columns = mesh.shape["row"], mesh.shape["col"]
    levels = (rows_ * columns).bit_length() - 1
    both = ("row", "col")
    placed = (
        P(both, None, None),
        P(both, None, None),
        P(both, None, None, None),
        P(both, None, None, None),
        P(both, None, None, None, None),
        P(both, None, None, None, None),
        P(both, None, None, None, None),
    )
    return jax.shard_map(
        functools.partial(shards, levels, columns),
        mesh=mesh, in_specs=placed, out_specs=P(both, None, None), check_vma=False,
    )
```

```python
import functools

import jax
import jax.numpy as jnp
from jax import lax
from jax.experimental import pallas as pl
from jax.experimental.pallas import tpu as pltpu
from jax.sharding import PartitionSpec as P

MESH = pl.DeviceIdType.MESH
BF16 = jnp.bfloat16
F32 = jnp.float32
ASC, DESC, COUP, SIB = 0, 1, 2, 3


def mm(a, b, ca=1, cb=0):
    return lax.dot_general(
        a.astype(BF16), b.astype(BF16), (((ca,), (cb,)), ((), ())), preferred_element_type=F32
    )


def rows(values):
    return jnp.concatenate([v.astype(BF16) for v in values], 0)


def cols(values):
    return jnp.concatenate([v.astype(BF16) for v in values], 1)


def split(levels):
    cuts = [0, *range(1, levels + 1, 2)]
    return list(zip(cuts[:-1], cuts[1:]))


def kept(levels):
    groups = split(levels)
    firsts = [lo + 1 for lo, _ in groups[1:-1]]
    found = [(COUP, h) for h in range(1, levels + 1)]
    found += [(kind, h) for h in range(1, levels - 1) for kind in (ASC, DESC)]
    return found + [(SIB, h) for h in firsts]


def tree_kernel(
    levels, columns,
    da_ref, db_ref, inner_ref, outer_ref, asc_ref, desc_ref, coup_ref, o_ref,
    da, db, inner, outer, asc, desc, coup, base, left, right,
    table, t_out, n_out, d_in, cross, near,
    load_sem, w_send, w_recv, d_send, d_recv, c_recv, told_sem,
):
    pos = lax.axis_index("row") * columns + lax.axis_index("col")
    bit = [pos // 2**i % 2 for i in range(levels)]
    groups = split(levels)
    final = len(groups) - 1
    top = {h: g for g, (lo, hi) in enumerate(groups) for h in range(lo + 1, hi + 1)}
    late = list(range(groups[final][0] + 1, levels + 1))
    r, m = asc.shape[-1], da.shape[-1]
    place = {item: n for n, item in enumerate(kept(levels))}

    def neighbour(g, f, core=0):
        lo, hi = groups[g]
        other = pos + core * (1 - 2 * bit[0])
        for i in range(lo, hi):
            if f >> (i - lo) & 1:
                other = other + 2**i * (1 - 2 * bit[i])
        return other // columns, other % columns

    def flips(g):
        lo, hi = groups[g]
        return [f for f in (1, 3, 2) if f < 2 ** (hi - lo)]

    def ones(n):
        return pos % 2**n == 2**n - 1

    def owner(h):
        return pos % 2**h == 2 ** (h - 1) - 1

    barrier = pltpu.get_barrier_semaphore()
    hub, side = ones(1), jnp.logical_not(ones(1))
    mate = neighbour(0, 1)
    lower = [neighbour(g, f) for g in range(1, final) for f in flips(g)]
    upper = [neighbour(final, f, 1) for f in flips(final)]

    def greet(others):
        for other in others:
            pl.semaphore_signal(barrier, inc=1, device_id=other, device_id_type=MESH)

    greet([mate])

    @pl.when(hub)
    def _():
        greet(lower)
        greet(upper)

    pl.when(side)(lambda: greet([neighbour(final, f) for f in flips(final)]))

    def load(src, dst, n):
        pltpu.make_async_copy(src, dst, load_sem.at[n]).start()

    def landed(ref, sem):
        pltpu.make_async_copy(ref, ref, sem).wait()

    load(asc_ref.at[0], asc, 0)
    load(inner_ref, inner, 1)

    def slot(kind, h):
        return table.at[place[kind, h]]

    def weight(kind, h, n):
        return table[place[kind, h], n]

    def targets(kind, h, g):
        lo, _ = groups[g]
        if g < top[h]:
            return [(f, kind, slot(kind, h)) for f in flips(g)]
        found = []
        for f in flips(g):
            beyond = f >> (h - lo)
            if kind == ASC:
                found.append((f, SIB if beyond else ASC, slot(ASC, h)))
            elif beyond:
                continue
            elif kind == COUP and f >> (h - 1 - lo) & 1:
                found.append((f, COUP, coup.at[1, 1:3]))
            else:
                found.append((f, kind, slot(kind, h)))
        return found

    def copies(kind, h, g):
        return [
            pltpu.make_async_remote_copy(
                src_ref=src, dst_ref=slot(to, h),
                send_sem=w_send.at[g], recv_sem=w_recv.at[place[to, h]],
                device_id=neighbour(g, f), device_id_type=MESH,
            )
            for f, to, src in targets(kind, h, g)
        ]

    def give(kind, h, gs):
        @pl.when(owner(h))
        def _():
            for g in gs:
                for copy in copies(kind, h, g):
                    copy.start()

    def down(kind, h):
        return list(reversed(range(int(kind in (ASC, SIB) and h > 1), top[h] + 1)))

    def take(kind, h, who=None):
        waits = jnp.logical_not(owner(h)) if kind != SIB else None
        if who is not None:
            waits = who if waits is None else waits & who

        def body():
            pltpu.make_async_copy(slot(kind, h), slot(kind, h), w_recv.at[place[kind, h]]).wait()
            for g in [g for g in down(kind, h) if g < top[h]]:
                @pl.when(ones(groups[g][1]))
                def _(g=g):
                    for copy in copies(kind, h, g):
                        copy.start()

        if waits is None:
            body()
        else:
            pl.when(waits)(body)

    def remote(g, src, dst, recv, to):
        return pltpu.make_async_remote_copy(
            src_ref=src, dst_ref=dst, send_sem=d_send.at[0], recv_sem=recv,
            device_id=to, device_id_type=MESH,
        )

    def term_sem(g, f):
        return d_recv.at[g + int(g == final and f == 3)]

    def send_term(g, f, core=0):
        at = f + 4 * core if g == 1 else f
        remote(g, t_out.at[g], d_in.at[g, at], term_sem(g, f), neighbour(g, f, core)).start()

    def send_value(g, core=0):
        h = groups[g][0] + 1
        remote(g, n_out.at[g], cross.at[h], c_recv.at[h - 1], neighbour(g, 1, core)).start()

    def term_in(g, f):
        landed(d_in.at[g, f], term_sem(g, f))

    def value_in(h):
        landed(cross.at[h], c_recv.at[h - 1])

    def pass_value(h):
        remote(top[h], cross.at[h], cross.at[h], c_recv.at[h - 1], mate).start()

    def pass_term(g, f):
        remote(g, d_in.at[g, f], d_in.at[g, f], term_sem(g, f), mate).start()

    central = ones(groups[final][0])
    ends = bit[levels - 1] == bit[levels - 2]

    landed(asc, load_sem.at[0])
    for h in range(1, levels - 1):
        @pl.when(owner(h))
        def _(h=h):
            table[place[ASC, h], 0] = asc[3, 0].T
            table[place[ASC, h], 1] = asc[3, 1]

    def tell_mate():
        pl.semaphore_signal(told_sem, inc=1, device_id=mate, device_id_type=MESH)

    @pl.when(hub)
    def _():
        pl.semaphore_wait(barrier, 1 + len(lower))
        tell_mate()

    pl.when(side)(lambda: pl.semaphore_wait(told_sem, 1))
    for h in range(1, levels - 1):
        give(ASC, h, down(ASC, h))
    landed(inner, load_sem.at[1])
    load(coup_ref.at[0], coup, 2)
    load(desc_ref.at[0], desc, 2)
    load(da_ref, da, 3)
    load(db_ref, db, 3)
    load(outer_ref, outer, 4)
    turned = cols([asc[u, 0].T for u in range(2)])
    lifted_left = mm(asc[2, 0].T, turned).astype(BF16)
    lifted_right = mm(rows([asc[u, 1] for u in range(2)]), asc[2, 1])
    factors = [cols([asc[u, 1], lifted_right[u * r:(u + 1) * r]]) for u in range(2)]
    leaf = [mm(inner[u, 0], inner[u, 1], 0, 0).astype(BF16) for u in range(2)]
    half = rows([mm(leaf[u], factors[u]) for u in range(2)])
    term = mm(lifted_left, half[:, r:]).astype(BF16)
    n_out[0] = mm(turned, half[:, :r]).astype(BF16)
    t_out[0] = term
    pl.when(side)(lambda: send_term(0, 1))
    take(ASC, 1)
    t_out[1] = mm(weight(ASC, 1, 0), mm(term, weight(ASC, 1, 1))).astype(BF16)

    @pl.when(hub)
    def _():
        for f in flips(1):
            send_term(1, f)

    @pl.when(side)
    def _():
        for f in flips(1):
            send_term(1, f, 1)
        remote(1, t_out.at[1], d_in.at[1, 4], term_sem(1, 1), mate).start()

    send_value(0)
    landed(base.at[:16 * r * r // (2 * m)], load_sem.at[2])
    for h in reversed(range(1, levels + 1)):
        @pl.when(owner(h))
        def _(h=h):
            table[place[COUP, h], 0] = coup[1, 0]
            table[place[COUP, h], 1] = coup[1, 3]
            if h < levels - 1:
                table[place[DESC, h]] = desc[3]

        if h == 1:
            give(COUP, 1, [0])
            give(DESC, 1, [0])

    @pl.when(side)
    def _():
        pl.semaphore_wait(barrier, 1 + 2 * len(upper))
        tell_mate()

    left_chain = rows([desc[u, 0] for u in range(2)])
    right_chain = rows([desc[u, 1] for u in range(2)])

    def factors(h, left_chain, right_chain):
        before = mm(left_chain, weight(COUP, h, 0)).astype(BF16)
        return before, mm(weight(COUP, h, 1), right_chain, 1, 1).astype(BF16)

    def couple(value, before, after):
        spread = mm(value, after).astype(BF16)
        for u in range(2):
            near[u] += mm(before[u * r:(u + 1) * r], spread[:, u * r:(u + 1) * r])

    gives_top = owner(late[0]) | owner(late[1])

    @pl.when(gives_top)
    def _():
        pl.semaphore_wait(told_sem, 1)
        for h in reversed(late):
            give(COUP, h, [final])

    @pl.when(hub)
    def _():
        term_in(0, 1)
        n_out[1] = (t_out[0].astype(F32) + d_in[0, 1].astype(F32)).astype(BF16)

    pl.when(hub)(lambda: send_value(1))
    for h in range(2, levels - 1):
        give(COUP, h, down(COUP, h))
        give(DESC, h, down(DESC, h))
    for h in late:
        give(COUP, h, down(COUP, h)[1:])
    landed(base, load_sem.at[3])
    for u in range(2):
        base[u * m:(u + 1) * m] = mm(da[u], db[u])

    @pl.when(central)
    def _():
        for h in late:
            take(COUP, h)

    near[0] = mm(mm(coup[0, 0], leaf[1]), coup[0, 3])
    near[1] = mm(mm(coup[0, 1], leaf[0]), coup[0, 2])
    value_in(1)
    take(COUP, 1)
    take(DESC, 1)
    couple(cross[1], *factors(1, left_chain, right_chain))
    left_chain = mm(left_chain, desc[2, 0]).astype(BF16)
    right_chain = mm(right_chain, desc[2, 1]).astype(BF16)

    @pl.when(hub)
    def _():
        for h in range(2, levels - 1):
            take(ASC, h)
            if (SIB, h) in place:
                take(SIB, h)

    @pl.when(hub)
    def _():
        for g in range(1, final):
            lo, hi = groups[g]
            up_left = cols([weight(ASC, lo + 1, 0), weight(SIB, lo + 1, 0)])
            up_right = [weight(ASC, lo + 1, 1), weight(SIB, lo + 1, 1)]
            far_left = mm(weight(ASC, hi, 0), up_left).astype(BF16)
            far_right = mm(rows(up_right), weight(ASC, hi, 1))
            both = [cols([far_right[b * r:(b + 1) * r], up_right[b]]) for b in range(2)]
            here, there = ([1], [2, 3]) if g > 1 else ([4, 1, 5], [2, 6, 3, 7])
            landed(d_in.at[g, 1:1 + len(here + there)], term_sem(g, 1))
            own = sum((d_in[g, n].astype(F32) for n in here), t_out[g].astype(F32)).astype(BF16)
            other = sum(d_in[g, n].astype(F32) for n in there).astype(BF16)
            half = rows([mm(own, both[0]), mm(other, both[1])])
            t_out[g + 1] = mm(far_left, half[:, :r]).astype(BF16)
            if g + 1 == final:
                pl.when(jnp.logical_not(gives_top))(lambda: pl.semaphore_wait(told_sem, 1))
                pl.when(ends)(lambda: send_term(final, 3, 1))
                send_term(final, 3)
                send_term(final, 2)
                send_term(final, 2, 1)
            else:
                for f in flips(g + 1):
                    send_term(g + 1, f)
            n_out[g + 1] = mm(up_left, half[:, r:]).astype(BF16)
            send_value(g + 1)
            if g + 1 == final:
                send_value(final, 1)
            cross[lo + 2] = other
            pass_value(lo + 2)
            value_in(lo + 1)
            pass_value(lo + 1)

    near_levels = range(2, late[0])
    landed(outer, load_sem.at[4])
    ready, chains = {}, {}
    for h in near_levels:
        if h > 2:
            if h > 3:
                take(DESC, h - 2)
            left_chain = mm(left_chain, weight(DESC, h - 2, 0)).astype(BF16)
            right_chain = mm(right_chain, weight(DESC, h - 2, 1)).astype(BF16)
        chains[h] = left_chain, right_chain
        if h < late[0] - 1:
            take(COUP, h)
            ready[h] = factors(h, *chains[h])
    if late[0] > 3:
        take(DESC, late[0] - 2)
    left_chain = mm(left_chain, weight(DESC, late[0] - 2, 0)).astype(BF16)
    right_chain = mm(right_chain, weight(DESC, late[0] - 2, 1)).astype(BF16)
    left_base = [mm(outer[u, 0], left_chain[u * r:(u + 1) * r]).astype(BF16) for u in range(2)]
    right_base = [mm(outer[u, 1], right_chain[u * r:(u + 1) * r]).astype(BF16) for u in range(2)]
    take(COUP, late[0] - 1)
    ready[late[0] - 1] = factors(late[0] - 1, *chains[late[0] - 1])

    @pl.when(side)
    def _():
        for h in near_levels:
            value_in(h)

    for h in near_levels:
        couple(cross[h], *ready[h])
    for u in range(2):
        base[u * m:(u + 1) * m] += mm(mm(outer[u, 0], near[u]), outer[u, 1], 1, 1)
    take(DESC, late[1] - 2)
    for h in late:
        take(COUP, h, jnp.logical_not(central))
    first = cols([weight(COUP, late[0], 0), mm(weight(DESC, late[1] - 2, 0), weight(COUP, late[1], 0))])
    second = rows([
        weight(COUP, late[0], 1),
        mm(weight(COUP, late[1], 1), weight(DESC, late[1] - 2, 1), 1, 1),
    ])
    for u in range(2):
        left[u] = mm(left_base[u], first).astype(BF16)
        right[u] = mm(second, right_base[u], 1, 1).astype(BF16)

    value_in(late[0])
    term_in(final, 2)
    term_in(final, 3)
    pl.when(hub & jnp.logical_not(ends))(lambda: pass_term(final, 3))

    last = (d_in[final, 2].astype(F32) + d_in[final, 3].astype(F32)).astype(BF16)
    zero = jnp.zeros_like(last)
    blocks = rows([cols([cross[late[0]], zero]), cols([zero, last])])
    for u in range(2):
        o_ref[u] = (base[u * m:(u + 1) * m] + mm(mm(left[u], blocks), right[u])).astype(BF16)

    rows_each = r * r // (2 * m)
    pl.when(side)(lambda: landed(base.at[:6 * rows_each], d_send.at[0]))
    pl.when(hub)(lambda: landed(base.at[:(1 + 6 * final) * rows_each], d_send.at[0]))
    for k in range(levels + 1):
        @pl.when(owner(k + 1) if k < levels else ones(levels))
        def _(k=k):
            for g in range(final + 1):
                units = 0
                for kind, h in place:
                    if g not in down(kind, h):
                        continue
                    if kind != SIB and g == top[h] and k == h - 1 or g < top[h] and k >= groups[g][1]:
                        units += len(targets(kind, h, g))
                if units:
                    landed(base.at[:units * (r * r // m)], w_send.at[g])


def shards(levels, columns, dense_a, dense_b, inner, outer, ascent, descent, couplings):
    r = ascent.shape[-1]
    m = dense_a.shape[-1]
    arrays = (dense_a, dense_b, inner, outer, ascent, descent, couplings)
    vmem = pltpu.VMEM
    dma = pltpu.SemaphoreType.DMA
    groups = split(levels)
    n = len(groups)
    return pl.pallas_call(
        functools.partial(tree_kernel, levels, columns),
        out_shape=jax.ShapeDtypeStruct(dense_a.shape, BF16),
        in_specs=[pl.BlockSpec(memory_space=pltpu.HBM)] * 7,
        out_specs=pl.BlockSpec(memory_space=pltpu.VMEM),
        scratch_shapes=[
            vmem(dense_a.shape, BF16),
            vmem(dense_b.shape, BF16),
            vmem(inner.shape, BF16),
            vmem(outer.shape, BF16),
            vmem(ascent.shape[1:], BF16),
            vmem(descent.shape[1:], BF16),
            vmem(couplings.shape[1:], BF16),
            vmem((2 * m, m), F32),
            vmem((2, m, 2 * r), BF16),
            vmem((2, 2 * r, m), BF16),
            vmem((len(kept(levels)), 2, r, r), BF16),
            vmem((n, r, r), BF16),
            vmem((n, r, r), BF16),
            vmem((n, 8, r, r), BF16),
            vmem((levels, r, r), BF16),
            vmem((2, r, r), F32),
            dma((5,)),
            dma((n,)),
            dma((len(kept(levels)),)),
            dma((1,)),
            dma((n + 1,)),
            dma((levels - 1,)),
            pltpu.SemaphoreType.REGULAR,
        ],
        compiler_params=pltpu.CompilerParams(collective_id=0, has_side_effects=True, vmem_limit_bytes=24 * 2**20),
    )(*(pltpu.with_memory_space_constraint(x, pltpu.HBM) for x in arrays))


def solution(mesh):
    rows_, columns = mesh.shape["row"], mesh.shape["col"]
    levels = (rows_ * columns).bit_length() - 1
    both = ("row", "col")
    placed = (
        P(both, None, None),
        P(both, None, None),
        P(both, None, None, None),
        P(both, None, None, None),
        P(both, None, None, None, None),
        P(both, None, None, None, None),
        P(both, None, None, None, None),
    )
    return jax.shard_map(
        functools.partial(shards, levels, columns),
        mesh=mesh, in_specs=placed, out_specs=P(both, None, None), check_vma=False,
    )
```

```python
import functools

import jax
import jax.numpy as jnp
from jax import lax
from jax.experimental import pallas as pl
from jax.experimental.pallas import tpu as pltpu
from jax.sharding import PartitionSpec as P

MESH = pl.DeviceIdType.MESH
BF16 = jnp.bfloat16
F32 = jnp.float32
ASC, DESC, COUP, SIB = 0, 1, 2, 3


def mm(a, b, ca=1, cb=0):
    return lax.dot_general(
        a.astype(BF16), b.astype(BF16), (((ca,), (cb,)), ((), ())), preferred_element_type=F32
    )


def rows(values):
    return jnp.concatenate([v.astype(BF16) for v in values], 0)


def cols(values):
    return jnp.concatenate([v.astype(BF16) for v in values], 1)


def split(levels):
    cuts = [0, *range(1, levels + 1, 2)]
    return list(zip(cuts[:-1], cuts[1:]))


def kept(levels):
    groups = split(levels)
    firsts = [lo + 1 for lo, _ in groups[1:-1]]
    found = [(COUP, h) for h in range(1, levels + 1)]
    found += [(kind, h) for h in range(1, levels - 1) for kind in (ASC, DESC)]
    return found + [(SIB, h) for h in firsts]


def tree_kernel(
    levels, columns,
    da_ref, db_ref, inner_ref, outer_ref, asc_ref, desc_ref, coup_ref, base, left, right, ends_ref,
    da, db, inner, outer, asc, desc, coup,
    table, t_out, n_out, d_in, cross, near,
    load_sem, w_send, w_recv, d_send, d_recv, c_recv, told_sem, pair_sem,
):
    pos = lax.axis_index("row") * columns + lax.axis_index("col")
    bit = [pos // 2**i % 2 for i in range(levels)]
    groups = split(levels)
    final = len(groups) - 1
    top = {h: g for g, (lo, hi) in enumerate(groups) for h in range(lo + 1, hi + 1)}
    late = list(range(groups[final][0] + 1, levels + 1))
    r, m = asc.shape[-1], da.shape[-1]
    place = {item: n for n, item in enumerate(kept(levels))}

    def neighbour(g, f, core=0):
        lo, hi = groups[g]
        other = pos + core * (1 - 2 * bit[0])
        for i in range(lo, hi):
            if f >> (i - lo) & 1:
                other = other + 2**i * (1 - 2 * bit[i])
        return other // columns, other % columns

    def flips(g):
        lo, hi = groups[g]
        return [f for f in (1, 3, 2) if f < 2 ** (hi - lo)]

    def ones(n):
        return pos % 2**n == 2**n - 1

    def owner(h):
        return pos % 2**h == 2 ** (h - 1) - 1

    barrier = pltpu.get_barrier_semaphore()
    hub, side = ones(1), jnp.logical_not(ones(1))
    mate = neighbour(0, 1)
    lower = [neighbour(g, f) for g in range(1, final) for f in flips(g)]
    upper = [neighbour(final, f, 1) for f in flips(final)]

    def greet(others):
        for other in others:
            pl.semaphore_signal(barrier, inc=1, device_id=other, device_id_type=MESH)

    greet([mate])

    @pl.when(hub)
    def _():
        greet(lower)
        greet(upper)


    def load(src, dst, n):
        pltpu.make_async_copy(src, dst, load_sem.at[n]).start()

    def landed(ref, sem):
        pltpu.make_async_copy(ref, ref, sem).wait()

    load(asc_ref.at[0], asc, 0)
    load(inner_ref, inner, 1)

    def slot(kind, h):
        return table.at[place[kind, h]]

    def weight(kind, h, n):
        return table[place[kind, h], n]

    def targets(kind, h, g):
        lo, _ = groups[g]
        if g < top[h]:
            return [(f, kind, slot(kind, h)) for f in flips(g)]
        found = []
        for f in flips(g):
            beyond = f >> (h - lo)
            if kind == ASC:
                found.append((f, SIB if beyond else ASC, slot(ASC, h)))
            elif beyond:
                continue
            elif kind == COUP and f >> (h - 1 - lo) & 1:
                found.append((f, COUP, coup.at[1, 1:3]))
            else:
                found.append((f, kind, slot(kind, h)))
        return found

    def copies(kind, h, g):
        return [
            pltpu.make_async_remote_copy(
                src_ref=src, dst_ref=slot(to, h),
                send_sem=w_send.at[g], recv_sem=w_recv.at[place[to, h]],
                device_id=neighbour(g, f), device_id_type=MESH,
            )
            for f, to, src in targets(kind, h, g)
        ]

    def give(kind, h, gs):
        @pl.when(owner(h))
        def _():
            for g in gs:
                for copy in copies(kind, h, g):
                    copy.start()

    def down(kind, h):
        return list(reversed(range(int(kind in (ASC, SIB) and h > 1), top[h] + 1)))

    def take(kind, h, who=None):
        waits = jnp.logical_not(owner(h)) if kind != SIB else None
        if who is not None:
            waits = who if waits is None else waits & who

        def body():
            pltpu.make_async_copy(slot(kind, h), slot(kind, h), w_recv.at[place[kind, h]]).wait()
            for g in [g for g in down(kind, h) if g < top[h]]:
                @pl.when(ones(groups[g][1]))
                def _(g=g):
                    for copy in copies(kind, h, g):
                        copy.start()

        if waits is None:
            body()
        else:
            pl.when(waits)(body)

    def remote(g, src, dst, recv, to):
        return pltpu.make_async_remote_copy(
            src_ref=src, dst_ref=dst, send_sem=d_send.at[0], recv_sem=recv,
            device_id=to, device_id_type=MESH,
        )

    def term_sem(g, f):
        return d_recv.at[g + int(g == final and f == 3)]

    def send_term(g, f, core=0):
        at = f + 4 * core if g == 1 else f
        remote(g, t_out.at[g], d_in.at[g, at], term_sem(g, f), neighbour(g, f, core)).start()

    def send_value(g, core=0):
        h = groups[g][0] + 1
        remote(g, n_out.at[g], cross.at[h], c_recv.at[h - 1], neighbour(g, 1, core)).start()

    def term_in(g, f):
        landed(d_in.at[g, f], term_sem(g, f))

    def value_in(h):
        landed(cross.at[h], c_recv.at[h - 1])

    def pass_value(h):
        remote(top[h], cross.at[h], cross.at[h], c_recv.at[h - 1], mate).start()

    def pass_term(g, f):
        remote(g, d_in.at[g, f], d_in.at[g, f], term_sem(g, f), mate).start()

    central = ones(groups[final][0])
    ends = bit[levels - 1] == bit[levels - 2]

    landed(asc, load_sem.at[0])
    for h in range(1, levels - 1):
        @pl.when(owner(h))
        def _(h=h):
            table[place[ASC, h], 0] = asc[3, 0].T
            table[place[ASC, h], 1] = asc[3, 1]

    def tell_mate():
        pl.semaphore_signal(told_sem, inc=1, device_id=mate, device_id_type=MESH)

    @pl.when(hub)
    def _():
        pl.semaphore_wait(barrier, 1 + len(lower))
        tell_mate()

    pl.when(side)(lambda: pl.semaphore_wait(told_sem, 1))
    for h in range(1, levels - 1):
        give(ASC, h, down(ASC, h))
    landed(inner, load_sem.at[1])
    load(coup_ref.at[0], coup, 2)
    load(desc_ref.at[0], desc, 2)
    load(da_ref, da, 3)
    load(db_ref, db, 3)
    load(outer_ref, outer, 4)
    turned = cols([asc[u, 0].T for u in range(2)])
    lifted_left = mm(asc[2, 0].T, turned).astype(BF16)
    lifted_right = mm(rows([asc[u, 1] for u in range(2)]), asc[2, 1])
    factors = [cols([asc[u, 1], lifted_right[u * r:(u + 1) * r]]) for u in range(2)]
    leaf = [mm(inner[u, 0], inner[u, 1], 0, 0).astype(BF16) for u in range(2)]
    half = rows([mm(leaf[u], factors[u]) for u in range(2)])
    term = mm(lifted_left, half[:, r:]).astype(BF16)
    n_out[0] = mm(turned, half[:, :r]).astype(BF16)
    t_out[0] = term
    pl.when(side)(lambda: send_term(0, 1))
    take(ASC, 1)
    t_out[1] = mm(weight(ASC, 1, 0), mm(term, weight(ASC, 1, 1))).astype(BF16)

    @pl.when(hub)
    def _():
        for f in (3, 1, 2):
            send_term(1, f)

    @pl.when(side)
    def _():
        for f in (3, 1, 2):
            send_term(1, f, 1)
        remote(1, t_out.at[1], d_in.at[1, 4], term_sem(1, 1), mate).start()

    send_value(0)
    landed(base.at[:16 * r * r // (2 * m)], load_sem.at[2])
    for h in reversed(range(1, levels + 1)):
        @pl.when(owner(h))
        def _(h=h):
            table[place[COUP, h], 0] = coup[1, 0]
            table[place[COUP, h], 1] = coup[1, 3]
            if h < levels - 1:
                table[place[DESC, h]] = desc[3]

        if h == 1:
            give(COUP, 1, [0])
            give(DESC, 1, [0])

    @pl.when(side)
    def _():
        pl.semaphore_wait(barrier, 1 + len(upper))
        tell_mate()

    left_chain = rows([desc[u, 0] for u in range(2)])
    right_chain = rows([desc[u, 1] for u in range(2)])

    def factors(h, left_chain, right_chain):
        before = mm(left_chain, weight(COUP, h, 0)).astype(BF16)
        return before, mm(weight(COUP, h, 1), right_chain, 1, 1).astype(BF16)

    def couple(value, before, after):
        spread = mm(value, after).astype(BF16)
        for u in range(2):
            near[u] += mm(before[u * r:(u + 1) * r], spread[:, u * r:(u + 1) * r])

    @pl.when(hub)
    def _():
        pl.semaphore_wait(told_sem, 1)
        for f in flips(final):
            pl.semaphore_signal(pair_sem, inc=1, device_id=neighbour(final, f), device_id_type=MESH)

    for h in reversed(late):
        give(COUP, h, [final])

    @pl.when(hub)
    def _():
        term_in(0, 1)
        n_out[1] = (t_out[0].astype(F32) + d_in[0, 1].astype(F32)).astype(BF16)

    landed(base, load_sem.at[3])
    for u in range(2):
        base[u * m:(u + 1) * m] = mm(da[u], db[u])
    pl.when(hub)(lambda: send_value(1))
    for h in range(2, levels - 1):
        give(COUP, h, down(COUP, h))
        give(DESC, h, down(DESC, h))
    for h in late:
        give(COUP, h, down(COUP, h)[1:])

    @pl.when(central)
    def _():
        for h in late:
            take(COUP, h)

    near[0] = mm(mm(coup[0, 0], leaf[1]), coup[0, 3])
    near[1] = mm(mm(coup[0, 1], leaf[0]), coup[0, 2])
    value_in(1)
    take(COUP, 1)
    take(DESC, 1)
    couple(cross[1], *factors(1, left_chain, right_chain))
    left_chain = mm(left_chain, desc[2, 0]).astype(BF16)
    right_chain = mm(right_chain, desc[2, 1]).astype(BF16)

    @pl.when(hub)
    def _():
        for h in range(2, levels - 1):
            take(ASC, h)
            if (SIB, h) in place:
                take(SIB, h)

    @pl.when(hub)
    def _():
        for g in range(1, final):
            lo, hi = groups[g]
            up_left = cols([weight(ASC, lo + 1, 0), weight(SIB, lo + 1, 0)])
            up_right = [weight(ASC, lo + 1, 1), weight(SIB, lo + 1, 1)]
            far_left = mm(weight(ASC, hi, 0), up_left).astype(BF16)
            far_right = mm(rows(up_right), weight(ASC, hi, 1))
            both = [cols([far_right[b * r:(b + 1) * r], up_right[b]]) for b in range(2)]
            here, there = ([1], [2, 3]) if g > 1 else ([4, 1, 5], [2, 6, 3, 7])
            landed(d_in.at[g, 1:1 + len(here + there)], term_sem(g, 1))
            own = sum((d_in[g, n].astype(F32) for n in here), t_out[g].astype(F32)).astype(BF16)
            other = sum(d_in[g, n].astype(F32) for n in there).astype(BF16)
            half = rows([mm(own, both[0]), mm(other, both[1])])
            t_out[g + 1] = mm(far_left, half[:, :r]).astype(BF16)
            if g + 1 == final:
                pl.semaphore_wait(pair_sem, len(upper))
                pl.when(ends)(lambda: send_term(final, 3, 1))
                send_term(final, 3)
                send_term(final, 2)
                send_term(final, 2, 1)
            else:
                for f in flips(g + 1):
                    send_term(g + 1, f)
            n_out[g + 1] = mm(up_left, half[:, r:]).astype(BF16)
            send_value(g + 1)
            if g + 1 == final:
                send_value(final, 1)
            cross[lo + 2] = other
            pass_value(lo + 2)
            value_in(lo + 1)
            pass_value(lo + 1)

    near_levels = range(2, late[0])
    landed(outer, load_sem.at[4])
    ready, chains = {}, {}
    for h in near_levels:
        if h > 2:
            if h > 3:
                take(DESC, h - 2)
            left_chain = mm(left_chain, weight(DESC, h - 2, 0)).astype(BF16)
            right_chain = mm(right_chain, weight(DESC, h - 2, 1)).astype(BF16)
        chains[h] = left_chain, right_chain
        if h < late[0] - 1:
            take(COUP, h)
            ready[h] = factors(h, *chains[h])
    if late[0] > 3:
        take(DESC, late[0] - 2)
    left_chain = mm(left_chain, weight(DESC, late[0] - 2, 0)).astype(BF16)
    right_chain = mm(right_chain, weight(DESC, late[0] - 2, 1)).astype(BF16)
    left_base = [mm(outer[u, 0], left_chain[u * r:(u + 1) * r]).astype(BF16) for u in range(2)]
    right_base = [mm(outer[u, 1], right_chain[u * r:(u + 1) * r]).astype(BF16) for u in range(2)]
    take(COUP, late[0] - 1)
    ready[late[0] - 1] = factors(late[0] - 1, *chains[late[0] - 1])

    @pl.when(side)
    def _():
        for h in near_levels:
            value_in(h)

    for h in near_levels:
        couple(cross[h], *ready[h])
    for u in range(2):
        base[u * m:(u + 1) * m] += mm(mm(outer[u, 0], near[u]), outer[u, 1], 1, 1)
    take(DESC, late[1] - 2)
    for h in late:
        take(COUP, h, jnp.logical_not(central))
    first = cols([weight(COUP, late[0], 0), mm(weight(DESC, late[1] - 2, 0), weight(COUP, late[1], 0))])
    second = rows([
        weight(COUP, late[0], 1),
        mm(weight(COUP, late[1], 1), weight(DESC, late[1] - 2, 1), 1, 1),
    ])
    for u in range(2):
        left[u] = mm(left_base[u], first).astype(BF16)
        right[u] = mm(second, right_base[u], 1, 1).astype(BF16)

    value_in(late[0])
    term_in(final, 2)
    term_in(final, 3)
    pl.when(hub & jnp.logical_not(ends))(lambda: pass_term(final, 3))

    ends_ref[0] = cross[late[0]]
    ends_ref[1] = (d_in[final, 2].astype(F32) + d_in[final, 3].astype(F32)).astype(BF16)

    rows_each = r * r // (2 * m)
    pl.when(side)(lambda: landed(base.at[:6 * rows_each], d_send.at[0]))
    pl.when(hub)(lambda: landed(base.at[:(1 + 6 * final) * rows_each], d_send.at[0]))
    for k in range(levels + 1):
        @pl.when(owner(k + 1) if k < levels else ones(levels))
        def _(k=k):
            for g in range(final + 1):
                units = 0
                for kind, h in place:
                    if g not in down(kind, h):
                        continue
                    if kind != SIB and g == top[h] and k == h - 1 or g < top[h] and k >= groups[g][1]:
                        units += len(targets(kind, h, g))
                if units:
                    landed(base.at[:units * (r * r // m)], w_send.at[g])


def last_kernel(base, left, right, ends_ref, o_ref, result, sem):
    m = result.shape[1]
    near, far = ends_ref[0], ends_ref[1]
    zero = jnp.zeros_like(far)
    blocks = rows([cols([near, zero]), cols([zero, far])])
    spread = [mm(left[u], blocks).astype(BF16) for u in range(2)]
    copies = []
    for u in range(2):
        for n in range(2):
            part = slice(n * m // 2, (n + 1) * m // 2)
            start = u * m + n * m // 2
            result[u, part] = (base[start:start + m // 2] + mm(spread[u][part], right[u])).astype(BF16)
            copies.append(pltpu.make_async_copy(result.at[u, part], o_ref.at[u, part], sem.at[2 * u + n]))
            copies[-1].start()
    for copy in copies:
        copy.wait()


def shards(levels, columns, dense_a, dense_b, inner, outer, ascent, descent, couplings):
    r = ascent.shape[-1]
    m = dense_a.shape[-1]
    arrays = (dense_a, dense_b, inner, outer, ascent, descent, couplings)
    vmem = pltpu.VMEM
    dma = pltpu.SemaphoreType.DMA
    groups = split(levels)
    n = len(groups)
    parts = pl.pallas_call(
        functools.partial(tree_kernel, levels, columns),
        out_shape=(
            jax.ShapeDtypeStruct((2 * m, m), F32),
            jax.ShapeDtypeStruct((2, m, 2 * r), BF16),
            jax.ShapeDtypeStruct((2, 2 * r, m), BF16),
            jax.ShapeDtypeStruct((2, r, r), BF16),
        ),
        in_specs=[pl.BlockSpec(memory_space=pltpu.HBM)] * 7,
        out_specs=(pl.BlockSpec(memory_space=pltpu.VMEM),) * 4,
        scratch_shapes=[
            vmem(dense_a.shape, BF16),
            vmem(dense_b.shape, BF16),
            vmem(inner.shape, BF16),
            vmem(outer.shape, BF16),
            vmem(ascent.shape[1:], BF16),
            vmem(descent.shape[1:], BF16),
            vmem(couplings.shape[1:], BF16),
            vmem((len(kept(levels)), 2, r, r), BF16),
            vmem((n, r, r), BF16),
            vmem((n, r, r), BF16),
            vmem((n, 8, r, r), BF16),
            vmem((levels, r, r), BF16),
            vmem((2, r, r), F32),
            dma((5,)),
            dma((n,)),
            dma((len(kept(levels)),)),
            dma((1,)),
            dma((n + 1,)),
            dma((levels - 1,)),
            pltpu.SemaphoreType.REGULAR,
            pltpu.SemaphoreType.REGULAR,
        ],
        compiler_params=pltpu.CompilerParams(collective_id=0, has_side_effects=True, vmem_limit_bytes=24 * 2**20),
    )(*(pltpu.with_memory_space_constraint(x, pltpu.HBM) for x in arrays))
    return pl.pallas_call(
        last_kernel,
        out_shape=jax.ShapeDtypeStruct(dense_a.shape, BF16),
        in_specs=[pl.BlockSpec(memory_space=pltpu.VMEM)] * 4,
        out_specs=pl.BlockSpec(memory_space=pltpu.HBM),
        scratch_shapes=[vmem(dense_a.shape, BF16), dma((4,))],
        compiler_params=pltpu.CompilerParams(vmem_limit_bytes=8 * 2**20),
    )(*parts)


def solution(mesh):
    rows_, columns = mesh.shape["row"], mesh.shape["col"]
    levels = (rows_ * columns).bit_length() - 1
    both = ("row", "col")
    placed = (
        P(both, None, None),
        P(both, None, None),
        P(both, None, None, None),
        P(both, None, None, None),
        P(both, None, None, None, None),
        P(both, None, None, None, None),
        P(both, None, None, None, None),
    )
    return jax.shard_map(
        functools.partial(shards, levels, columns),
        mesh=mesh, in_specs=placed, out_specs=P(both, None, None), check_vma=False,
    )
```

```python
import functools

import jax
import jax.numpy as jnp
from jax import lax
from jax.experimental import pallas as pl
from jax.experimental.pallas import tpu as pltpu
from jax.sharding import PartitionSpec as P

MESH = pl.DeviceIdType.MESH
BF16 = jnp.bfloat16
F32 = jnp.float32
ASC, DESC, COUP, SIB = 0, 1, 2, 3


def mm(a, b, ca=1, cb=0):
    return lax.dot_general(
        a.astype(BF16), b.astype(BF16), (((ca,), (cb,)), ((), ())), preferred_element_type=F32
    )


def rows(values):
    return jnp.concatenate([v.astype(BF16) for v in values], 0)


def cols(values):
    return jnp.concatenate([v.astype(BF16) for v in values], 1)


def split(levels):
    cuts = [0, *range(1, levels + 1, 2)]
    return list(zip(cuts[:-1], cuts[1:]))


def kept(levels):
    groups = split(levels)
    firsts = [lo + 1 for lo, _ in groups[1:-1]]
    found = [(COUP, h) for h in range(1, levels + 1)]
    found += [(kind, h) for h in range(1, levels - 1) for kind in (ASC, DESC)]
    return found + [(SIB, h) for h in firsts]


def tree_kernel(
    levels, columns,
    da_ref, db_ref, inner_ref, outer_ref, asc_ref, desc_ref, coup_ref, base, left, right, ends_ref,
    da, db, inner, outer, asc, desc, coup,
    table, t_out, n_out, d_in, cross, near,
    load_sem, w_send, w_recv, d_send, d_recv, c_recv, told_sem, pair_sem,
):
    pos = lax.axis_index("row") * columns + lax.axis_index("col")
    bit = [pos // 2**i % 2 for i in range(levels)]
    groups = split(levels)
    final = len(groups) - 1
    top = {h: g for g, (lo, hi) in enumerate(groups) for h in range(lo + 1, hi + 1)}
    late = list(range(groups[final][0] + 1, levels + 1))
    r, m = asc.shape[-1], da.shape[-1]
    place = {item: n for n, item in enumerate(kept(levels))}

    def neighbour(g, f, core=0):
        lo, hi = groups[g]
        other = pos + core * (1 - 2 * bit[0])
        for i in range(lo, hi):
            if f >> (i - lo) & 1:
                other = other + 2**i * (1 - 2 * bit[i])
        return other // columns, other % columns

    def flips(g):
        lo, hi = groups[g]
        return [f for f in (1, 3, 2) if f < 2 ** (hi - lo)]

    def ones(n):
        return pos % 2**n == 2**n - 1

    def owner(h):
        return pos % 2**h == 2 ** (h - 1) - 1

    barrier = pltpu.get_barrier_semaphore()
    hub, side = ones(1), jnp.logical_not(ones(1))
    mate = neighbour(0, 1)
    lower = [neighbour(g, f) for g in range(1, final) for f in flips(g)]
    upper = [neighbour(final, f, 1) for f in flips(final)]

    def greet(others):
        for other in others:
            pl.semaphore_signal(barrier, inc=1, device_id=other, device_id_type=MESH)

    greet([mate])

    @pl.when(hub)
    def _():
        greet(lower)
        greet(upper)


    def load(src, dst, n):
        pltpu.make_async_copy(src, dst, load_sem.at[n]).start()

    def landed(ref, sem):
        pltpu.make_async_copy(ref, ref, sem).wait()

    load(asc_ref.at[0], asc, 0)
    load(inner_ref, inner, 1)

    def slot(kind, h):
        return table.at[place[kind, h]]

    def weight(kind, h, n):
        return table[place[kind, h], n]

    def targets(kind, h, g):
        lo, _ = groups[g]
        if g < top[h]:
            return [(f, kind, slot(kind, h)) for f in flips(g)]
        found = []
        for f in flips(g):
            beyond = f >> (h - lo)
            if kind == ASC:
                found.append((f, SIB if beyond else ASC, slot(ASC, h)))
            elif beyond:
                continue
            elif kind == COUP and f >> (h - 1 - lo) & 1:
                found.append((f, COUP, coup.at[1, 1:3]))
            else:
                found.append((f, kind, slot(kind, h)))
        return found

    def copies(kind, h, g):
        return [
            pltpu.make_async_remote_copy(
                src_ref=src, dst_ref=slot(to, h),
                send_sem=w_send.at[g], recv_sem=w_recv.at[place[to, h]],
                device_id=neighbour(g, f), device_id_type=MESH,
            )
            for f, to, src in targets(kind, h, g)
        ]

    def give(kind, h, gs):
        @pl.when(owner(h))
        def _():
            for g in gs:
                for copy in copies(kind, h, g):
                    copy.start()

    def down(kind, h):
        return list(reversed(range(int(kind in (ASC, SIB) and h > 1), top[h] + 1)))

    def take(kind, h, who=None):
        waits = jnp.logical_not(owner(h)) if kind != SIB else None
        if who is not None:
            waits = who if waits is None else waits & who

        def body():
            pltpu.make_async_copy(slot(kind, h), slot(kind, h), w_recv.at[place[kind, h]]).wait()
            for g in [g for g in down(kind, h) if g < top[h]]:
                @pl.when(ones(groups[g][1]))
                def _(g=g):
                    for copy in copies(kind, h, g):
                        copy.start()

        if waits is None:
            body()
        else:
            pl.when(waits)(body)

    def remote(g, src, dst, recv, to):
        return pltpu.make_async_remote_copy(
            src_ref=src, dst_ref=dst, send_sem=d_send.at[0], recv_sem=recv,
            device_id=to, device_id_type=MESH,
        )

    def term_sem(g, f):
        return d_recv.at[g + int(g == final and f == 3)]

    def send_term(g, f, core=0):
        at = f + 4 * core if g == 1 else f
        remote(g, t_out.at[g], d_in.at[g, at], term_sem(g, f), neighbour(g, f, core)).start()

    def send_value(g, core=0):
        h = groups[g][0] + 1
        remote(g, n_out.at[g], cross.at[h], c_recv.at[h - 1], neighbour(g, 1, core)).start()

    def term_in(g, f):
        landed(d_in.at[g, f], term_sem(g, f))

    def value_in(h):
        landed(cross.at[h], c_recv.at[h - 1])

    def pass_value(h):
        remote(top[h], cross.at[h], cross.at[h], c_recv.at[h - 1], mate).start()

    def pass_term(g, f):
        remote(g, d_in.at[g, f], d_in.at[g, f], term_sem(g, f), mate).start()

    central = ones(groups[final][0])
    ends = bit[levels - 1] == bit[levels - 2]

    def tell_mate():
        pl.semaphore_signal(told_sem, inc=1, device_id=mate, device_id_type=MESH)

    @pl.when(hub)
    def _():
        pl.semaphore_wait(barrier, 1 + len(lower))
        tell_mate()

    landed(asc, load_sem.at[0])
    for h in range(1, levels - 1):
        @pl.when(owner(h))
        def _(h=h):
            table[place[ASC, h], 0] = asc[3, 0].T
            table[place[ASC, h], 1] = asc[3, 1]

    pl.when(side)(lambda: pl.semaphore_wait(told_sem, 1))
    for h in range(1, levels - 1):
        give(ASC, h, down(ASC, h))
    landed(inner, load_sem.at[1])
    load(coup_ref.at[0], coup, 2)
    load(desc_ref.at[0], desc, 2)
    load(da_ref, da, 3)
    load(db_ref, db, 3)
    load(outer_ref, outer, 4)
    turned = cols([asc[u, 0].T for u in range(2)])
    lifted_left = mm(asc[2, 0].T, turned).astype(BF16)
    lifted_right = mm(rows([asc[u, 1] for u in range(2)]), asc[2, 1])
    factors = [cols([asc[u, 1], lifted_right[u * r:(u + 1) * r]]) for u in range(2)]
    leaf = [mm(inner[u, 0], inner[u, 1], 0, 0).astype(BF16) for u in range(2)]
    half = rows([mm(leaf[u], factors[u]) for u in range(2)])
    term = mm(lifted_left, half[:, r:]).astype(BF16)
    n_out[0] = mm(turned, half[:, :r]).astype(BF16)
    t_out[0] = term
    pl.when(side)(lambda: send_term(0, 1))
    take(ASC, 1)
    t_out[1] = mm(weight(ASC, 1, 0), mm(term, weight(ASC, 1, 1))).astype(BF16)

    @pl.when(hub)
    def _():
        for f in (3, 1, 2):
            send_term(1, f)

    @pl.when(side)
    def _():
        for f in (3, 1, 2):
            send_term(1, f, 1)
        remote(1, t_out.at[1], d_in.at[1, 4], term_sem(1, 1), mate).start()

    send_value(0)
    landed(base.at[:16 * r * r // (2 * m)], load_sem.at[2])
    for h in reversed(range(1, levels + 1)):
        @pl.when(owner(h))
        def _(h=h):
            table[place[COUP, h], 0] = coup[1, 0]
            table[place[COUP, h], 1] = coup[1, 3]
            if h < levels - 1:
                table[place[DESC, h]] = desc[3]

        if h == 1:
            give(COUP, 1, [0])
            give(DESC, 1, [0])

    @pl.when(side)
    def _():
        pl.semaphore_wait(barrier, 1 + len(upper))
        tell_mate()

    left_chain = rows([desc[u, 0] for u in range(2)])
    right_chain = rows([desc[u, 1] for u in range(2)])

    def factors(h, left_chain, right_chain):
        before = mm(left_chain, weight(COUP, h, 0)).astype(BF16)
        return before, mm(weight(COUP, h, 1), right_chain, 1, 1).astype(BF16)

    def couple(value, before, after):
        spread = mm(value, after).astype(BF16)
        for u in range(2):
            near[u] += mm(before[u * r:(u + 1) * r], spread[:, u * r:(u + 1) * r])

    @pl.when(hub)
    def _():
        pl.semaphore_wait(told_sem, 1)
        for f in flips(final):
            pl.semaphore_signal(pair_sem, inc=1, device_id=neighbour(final, f), device_id_type=MESH)

    for h in reversed(late):
        give(COUP, h, [final])

    @pl.when(hub)
    def _():
        term_in(0, 1)
        n_out[1] = (t_out[0].astype(F32) + d_in[0, 1].astype(F32)).astype(BF16)

    landed(base, load_sem.at[3])
    for u in range(2):
        base[u * m:(u + 1) * m] = mm(da[u], db[u])
    pl.when(hub)(lambda: send_value(1))
    for h in range(2, levels - 1):
        give(COUP, h, down(COUP, h))
        give(DESC, h, down(DESC, h))
    for h in late:
        give(COUP, h, down(COUP, h)[1:])

    @pl.when(central)
    def _():
        for h in late:
            take(COUP, h)

    near[0] = mm(mm(coup[0, 0], leaf[1]), coup[0, 3])
    near[1] = mm(mm(coup[0, 1], leaf[0]), coup[0, 2])
    value_in(1)
    take(COUP, 1)
    take(DESC, 1)
    couple(cross[1], *factors(1, left_chain, right_chain))
    left_chain = mm(left_chain, desc[2, 0]).astype(BF16)
    right_chain = mm(right_chain, desc[2, 1]).astype(BF16)

    @pl.when(hub)
    def _():
        for h in range(2, levels - 1):
            take(ASC, h)
            if (SIB, h) in place:
                take(SIB, h)

    @pl.when(hub)
    def _():
        for g in range(1, final):
            lo, hi = groups[g]
            up_left = cols([weight(ASC, lo + 1, 0), weight(SIB, lo + 1, 0)])
            up_right = [weight(ASC, lo + 1, 1), weight(SIB, lo + 1, 1)]
            far_left = mm(weight(ASC, hi, 0), up_left).astype(BF16)
            far_right = mm(rows(up_right), weight(ASC, hi, 1))
            both = [cols([far_right[b * r:(b + 1) * r], up_right[b]]) for b in range(2)]
            here, there = ([1], [2, 3]) if g > 1 else ([4, 1, 5], [2, 6, 3, 7])
            landed(d_in.at[g, 1:1 + len(here + there)], term_sem(g, 1))
            own = sum((d_in[g, n].astype(F32) for n in here), t_out[g].astype(F32)).astype(BF16)
            other = sum(d_in[g, n].astype(F32) for n in there).astype(BF16)
            half = rows([mm(own, both[0]), mm(other, both[1])])
            t_out[g + 1] = mm(far_left, half[:, :r]).astype(BF16)
            if g + 1 == final:
                pl.semaphore_wait(pair_sem, len(upper))
                @pl.when(ends)
                def _():
                    for f, core in ((3, 1), (3, 0), (2, 1), (2, 0)):
                        send_term(final, f, core)

                @pl.when(jnp.logical_not(ends))
                def _():
                    for f, core in ((2, 1), (2, 0), (3, 0)):
                        send_term(final, f, core)

            else:
                for f in flips(g + 1):
                    send_term(g + 1, f)
            n_out[g + 1] = mm(up_left, half[:, r:]).astype(BF16)
            send_value(g + 1)
            if g + 1 == final:
                send_value(final, 1)
            cross[lo + 2] = other
            pass_value(lo + 2)
            value_in(lo + 1)
            pass_value(lo + 1)

    near_levels = range(2, late[0])
    landed(outer, load_sem.at[4])
    ready, chains = {}, {}
    for h in near_levels:
        if h > 2:
            if h > 3:
                take(DESC, h - 2)
            left_chain = mm(left_chain, weight(DESC, h - 2, 0)).astype(BF16)
            right_chain = mm(right_chain, weight(DESC, h - 2, 1)).astype(BF16)
        chains[h] = left_chain, right_chain
        if h < late[0] - 1:
            take(COUP, h)
            ready[h] = factors(h, *chains[h])
    if late[0] > 3:
        take(DESC, late[0] - 2)
    left_chain = mm(left_chain, weight(DESC, late[0] - 2, 0)).astype(BF16)
    right_chain = mm(right_chain, weight(DESC, late[0] - 2, 1)).astype(BF16)
    left_base = [mm(outer[u, 0], left_chain[u * r:(u + 1) * r]).astype(BF16) for u in range(2)]
    right_base = [mm(outer[u, 1], right_chain[u * r:(u + 1) * r]).astype(BF16) for u in range(2)]
    take(COUP, late[0] - 1)
    ready[late[0] - 1] = factors(late[0] - 1, *chains[late[0] - 1])

    @pl.when(side)
    def _():
        for h in near_levels:
            value_in(h)

    for h in near_levels:
        couple(cross[h], *ready[h])
    for u in range(2):
        base[u * m:(u + 1) * m] += mm(mm(outer[u, 0], near[u]), outer[u, 1], 1, 1)
    take(DESC, late[1] - 2)
    for h in late:
        take(COUP, h, jnp.logical_not(central))
    first = cols([weight(COUP, late[0], 0), mm(weight(DESC, late[1] - 2, 0), weight(COUP, late[1], 0))])
    second = rows([
        weight(COUP, late[0], 1),
        mm(weight(COUP, late[1], 1), weight(DESC, late[1] - 2, 1), 1, 1),
    ])
    for u in range(2):
        left[u] = mm(left_base[u], first).astype(BF16)
        right[u] = mm(second, right_base[u], 1, 1).astype(BF16)

    value_in(late[0])
    term_in(final, 2)
    term_in(final, 3)
    pl.when(hub & jnp.logical_not(ends))(lambda: pass_term(final, 3))

    ends_ref[0] = cross[late[0]]
    ends_ref[1] = (d_in[final, 2].astype(F32) + d_in[final, 3].astype(F32)).astype(BF16)

    rows_each = r * r // (2 * m)
    pl.when(side)(lambda: landed(base.at[:6 * rows_each], d_send.at[0]))
    pl.when(hub)(lambda: landed(base.at[:(1 + 6 * final) * rows_each], d_send.at[0]))
    for k in range(levels + 1):
        @pl.when(owner(k + 1) if k < levels else ones(levels))
        def _(k=k):
            for g in range(final + 1):
                units = 0
                for kind, h in place:
                    if g not in down(kind, h):
                        continue
                    if kind != SIB and g == top[h] and k == h - 1 or g < top[h] and k >= groups[g][1]:
                        units += len(targets(kind, h, g))
                if units:
                    landed(base.at[:units * (r * r // m)], w_send.at[g])


def last_kernel(base, left, right, ends_ref, o_ref, result, sem):
    m = result.shape[1]
    near, far = ends_ref[0], ends_ref[1]
    zero = jnp.zeros_like(far)
    blocks = rows([cols([near, zero]), cols([zero, far])])
    spread = [mm(left[u], blocks).astype(BF16) for u in range(2)]
    copies = []
    for u in range(2):
        for n in range(2):
            part = slice(n * m // 2, (n + 1) * m // 2)
            start = u * m + n * m // 2
            result[u, part] = (base[start:start + m // 2] + mm(spread[u][part], right[u])).astype(BF16)
            copies.append(pltpu.make_async_copy(result.at[u, part], o_ref.at[u, part], sem.at[2 * u + n]))
            copies[-1].start()
    for copy in copies:
        copy.wait()


def shards(levels, columns, dense_a, dense_b, inner, outer, ascent, descent, couplings):
    r = ascent.shape[-1]
    m = dense_a.shape[-1]
    arrays = (dense_a, dense_b, inner, outer, ascent, descent, couplings)
    vmem = pltpu.VMEM
    dma = pltpu.SemaphoreType.DMA
    groups = split(levels)
    n = len(groups)
    parts = pl.pallas_call(
        functools.partial(tree_kernel, levels, columns),
        out_shape=(
            jax.ShapeDtypeStruct((2 * m, m), F32),
            jax.ShapeDtypeStruct((2, m, 2 * r), BF16),
            jax.ShapeDtypeStruct((2, 2 * r, m), BF16),
            jax.ShapeDtypeStruct((2, r, r), BF16),
        ),
        in_specs=[pl.BlockSpec(memory_space=pltpu.HBM)] * 7,
        out_specs=(pl.BlockSpec(memory_space=pltpu.VMEM),) * 4,
        scratch_shapes=[
            vmem(dense_a.shape, BF16),
            vmem(dense_b.shape, BF16),
            vmem(inner.shape, BF16),
            vmem(outer.shape, BF16),
            vmem(ascent.shape[1:], BF16),
            vmem(descent.shape[1:], BF16),
            vmem(couplings.shape[1:], BF16),
            vmem((len(kept(levels)), 2, r, r), BF16),
            vmem((n, r, r), BF16),
            vmem((n, r, r), BF16),
            vmem((n, 8, r, r), BF16),
            vmem((levels, r, r), BF16),
            vmem((2, r, r), F32),
            dma((5,)),
            dma((n,)),
            dma((len(kept(levels)),)),
            dma((1,)),
            dma((n + 1,)),
            dma((levels - 1,)),
            pltpu.SemaphoreType.REGULAR,
            pltpu.SemaphoreType.REGULAR,
        ],
        compiler_params=pltpu.CompilerParams(collective_id=0, has_side_effects=True, vmem_limit_bytes=24 * 2**20),
    )(*(pltpu.with_memory_space_constraint(x, pltpu.HBM) for x in arrays))
    return pl.pallas_call(
        last_kernel,
        out_shape=jax.ShapeDtypeStruct(dense_a.shape, BF16),
        in_specs=[pl.BlockSpec(memory_space=pltpu.VMEM)] * 4,
        out_specs=pl.BlockSpec(memory_space=pltpu.HBM),
        scratch_shapes=[vmem(dense_a.shape, BF16), dma((4,))],
        compiler_params=pltpu.CompilerParams(vmem_limit_bytes=8 * 2**20),
    )(*parts)


def solution(mesh):
    rows_, columns = mesh.shape["row"], mesh.shape["col"]
    levels = (rows_ * columns).bit_length() - 1
    both = ("row", "col")
    placed = (
        P(both, None, None),
        P(both, None, None),
        P(both, None, None, None),
        P(both, None, None, None),
        P(both, None, None, None, None),
        P(both, None, None, None, None),
        P(both, None, None, None, None),
    )
    return jax.shard_map(
        functools.partial(shards, levels, columns),
        mesh=mesh, in_specs=placed, out_specs=P(both, None, None), check_vma=False,
    )
```

```python
import functools

import jax
import jax.numpy as jnp
from jax import lax
from jax.experimental import pallas as pl
from jax.experimental.pallas import tpu as pltpu
from jax.sharding import PartitionSpec as P

MESH = pl.DeviceIdType.MESH
BF16 = jnp.bfloat16
F32 = jnp.float32
ASC, DESC, COUP, SIB = 0, 1, 2, 3


def mm(a, b, ca=1, cb=0):
    return lax.dot_general(
        a.astype(BF16), b.astype(BF16), (((ca,), (cb,)), ((), ())), preferred_element_type=F32
    )


def rows(values):
    return jnp.concatenate([v.astype(BF16) for v in values], 0)


def cols(values):
    return jnp.concatenate([v.astype(BF16) for v in values], 1)


def split(levels):
    cuts = [0, *range(1, levels + 1, 2)]
    return list(zip(cuts[:-1], cuts[1:]))


def kept(levels):
    groups = split(levels)
    firsts = [lo + 1 for lo, _ in groups[1:-1]]
    found = [(COUP, h) for h in range(1, levels + 1)]
    found += [(kind, h) for h in range(1, levels - 1) for kind in (ASC, DESC)]
    return found + [(SIB, h) for h in firsts]


def tree_kernel(
    levels, columns,
    da_ref, db_ref, inner_ref, outer_ref, asc_ref, desc_ref, coup_ref, base, left, right, ends_ref,
    da, db, inner, outer, asc, desc, coup,
    table, t_out, n_out, d_in, cross, near,
    load_sem, w_send, w_recv, d_send, d_recv, c_recv, told_sem, pair_sem,
):
    pos = lax.axis_index("row") * columns + lax.axis_index("col")
    bit = [pos // 2**i % 2 for i in range(levels)]
    groups = split(levels)
    final = len(groups) - 1
    top = {h: g for g, (lo, hi) in enumerate(groups) for h in range(lo + 1, hi + 1)}
    late = list(range(groups[final][0] + 1, levels + 1))
    r, m = asc.shape[-1], da.shape[-1]
    place = {item: n for n, item in enumerate(kept(levels))}

    def neighbour(g, f, core=0):
        lo, hi = groups[g]
        other = pos + core * (1 - 2 * bit[0])
        for i in range(lo, hi):
            if f >> (i - lo) & 1:
                other = other + 2**i * (1 - 2 * bit[i])
        return other // columns, other % columns

    def flips(g):
        lo, hi = groups[g]
        return [f for f in (1, 3, 2) if f < 2 ** (hi - lo)]

    def ones(n):
        return pos % 2**n == 2**n - 1

    def owner(h):
        return pos % 2**h == 2 ** (h - 1) - 1

    barrier = pltpu.get_barrier_semaphore()
    hub, side = ones(1), jnp.logical_not(ones(1))
    mate = neighbour(0, 1)
    lower = [neighbour(g, f) for g in range(1, final) for f in flips(g)]
    upper = [neighbour(final, f, 1) for f in flips(final)]

    def greet(others):
        for other in others:
            pl.semaphore_signal(barrier, inc=1, device_id=other, device_id_type=MESH)

    greet([mate])

    @pl.when(hub)
    def _():
        greet(lower)
        greet(upper)


    def load(src, dst, n):
        pltpu.make_async_copy(src, dst, load_sem.at[n]).start()

    def landed(ref, sem):
        pltpu.make_async_copy(ref, ref, sem).wait()

    load(asc_ref.at[0], asc, 0)
    load(inner_ref, inner, 1)

    def slot(kind, h):
        return table.at[place[kind, h]]

    def weight(kind, h, n):
        return table[place[kind, h], n]

    def targets(kind, h, g):
        lo, _ = groups[g]
        if g < top[h]:
            return [(f, kind, slot(kind, h)) for f in flips(g)]
        found = []
        for f in flips(g):
            beyond = f >> (h - lo)
            if kind == ASC:
                found.append((f, SIB if beyond else ASC, slot(ASC, h)))
            elif beyond:
                continue
            elif kind == COUP and f >> (h - 1 - lo) & 1:
                found.append((f, COUP, coup.at[1, 1:3]))
            else:
                found.append((f, kind, slot(kind, h)))
        return found

    def copies(kind, h, g):
        return [
            pltpu.make_async_remote_copy(
                src_ref=src, dst_ref=slot(to, h),
                send_sem=w_send.at[0], recv_sem=w_recv.at[place[COUP, 1] if (to, h) == (DESC, 1) else place[to, h]],
                device_id=neighbour(g, f), device_id_type=MESH,
            )
            for f, to, src in targets(kind, h, g)
        ]

    def give(kind, h, gs):
        @pl.when(owner(h))
        def _():
            for g in gs:
                for copy in copies(kind, h, g):
                    copy.start()

    def down(kind, h):
        return list(reversed(range(int(kind in (ASC, SIB) and h > 1), top[h] + 1)))

    def take(kind, h, who=None):
        waits = jnp.logical_not(owner(h)) if kind != SIB else None
        if who is not None:
            waits = who if waits is None else waits & who

        def body():
            pltpu.make_async_copy(slot(kind, h), slot(kind, h), w_recv.at[place[kind, h]]).wait()
            for g in [g for g in down(kind, h) if g < top[h]]:
                @pl.when(ones(groups[g][1]))
                def _(g=g):
                    for copy in copies(kind, h, g):
                        copy.start()

        if waits is None:
            body()
        else:
            pl.when(waits)(body)

    def remote(g, src, dst, recv, to):
        return pltpu.make_async_remote_copy(
            src_ref=src, dst_ref=dst, send_sem=d_send.at[0], recv_sem=recv,
            device_id=to, device_id_type=MESH,
        )

    def term_sem(g, f):
        return d_recv.at[g + int(g == final and f == 3)]

    def send_term(g, f, core=0):
        at = f + 4 * core if g == 1 else f
        remote(g, t_out.at[g], d_in.at[g, at], term_sem(g, f), neighbour(g, f, core)).start()

    def send_value(g, core=0):
        h = groups[g][0] + 1
        remote(g, n_out.at[g], cross.at[h], c_recv.at[h - 1], neighbour(g, 1, core)).start()

    def term_in(g, f):
        landed(d_in.at[g, f], term_sem(g, f))

    def value_in(h):
        landed(cross.at[h], c_recv.at[h - 1])

    def pass_value(h):
        remote(top[h], cross.at[h], cross.at[h], c_recv.at[h - 1], mate).start()

    def pass_term(g, f):
        remote(g, d_in.at[g, f], d_in.at[g, f], term_sem(g, f), mate).start()

    central = ones(groups[final][0])
    ends = bit[levels - 1] == bit[levels - 2]

    landed(asc, load_sem.at[0])
    for h in range(1, levels - 1):
        @pl.when(owner(h))
        def _(h=h):
            table[place[ASC, h], 0] = asc[3, 0].T
            table[place[ASC, h], 1] = asc[3, 1]

    def tell_mate():
        pl.semaphore_signal(told_sem, inc=1, device_id=mate, device_id_type=MESH)

    @pl.when(hub)
    def _():
        pl.semaphore_wait(barrier, 1 + len(lower))
        tell_mate()

    pl.when(side)(lambda: pl.semaphore_wait(told_sem, 1))
    for h in range(1, levels - 1):
        give(ASC, h, down(ASC, h))
    landed(inner, load_sem.at[1])
    load(coup_ref.at[0], coup, 2)
    load(desc_ref.at[0], desc, 2)
    load(da_ref, da, 3)
    load(db_ref, db, 3)
    load(outer_ref, outer, 4)
    turned = cols([asc[u, 0].T for u in range(2)])
    lifted_left = mm(asc[2, 0].T, turned).astype(BF16)
    lifted_right = mm(rows([asc[u, 1] for u in range(2)]), asc[2, 1])
    factors = [cols([asc[u, 1], lifted_right[u * r:(u + 1) * r]]) for u in range(2)]
    leaf = [mm(inner[u, 0], inner[u, 1], 0, 0).astype(BF16) for u in range(2)]
    half = rows([mm(leaf[u], factors[u]) for u in range(2)])
    term = mm(lifted_left, half[:, r:]).astype(BF16)
    n_out[0] = mm(turned, half[:, :r]).astype(BF16)
    t_out[0] = term
    pl.when(side)(lambda: send_term(0, 1))
    take(ASC, 1)
    t_out[1] = mm(weight(ASC, 1, 0), mm(term, weight(ASC, 1, 1))).astype(BF16)

    @pl.when(hub)
    def _():
        for f in (3, 1, 2):
            send_term(1, f)

    @pl.when(side)
    def _():
        for f in (3, 1, 2):
            send_term(1, f, 1)
        remote(1, t_out.at[1], d_in.at[1, 4], term_sem(1, 1), mate).start()

    send_value(0)
    landed(base.at[:16 * r * r // (2 * m)], load_sem.at[2])
    for h in reversed(range(1, levels + 1)):
        @pl.when(owner(h))
        def _(h=h):
            table[place[COUP, h], 0] = coup[1, 0]
            table[place[COUP, h], 1] = coup[1, 3]
            if h < levels - 1:
                table[place[DESC, h]] = desc[3]

        if h == 1:
            give(COUP, 1, [0])
            give(DESC, 1, [0])

    @pl.when(side)
    def _():
        pl.semaphore_wait(barrier, 1 + len(upper))
        tell_mate()

    left_chain = rows([desc[u, 0] for u in range(2)])
    right_chain = rows([desc[u, 1] for u in range(2)])

    def factors(h, left_chain, right_chain):
        before = mm(left_chain, weight(COUP, h, 0)).astype(BF16)
        return before, mm(weight(COUP, h, 1), right_chain, 1, 1).astype(BF16)

    def couple(value, before, after):
        spread = mm(value, after).astype(BF16)
        for u in range(2):
            near[u] += mm(before[u * r:(u + 1) * r], spread[:, u * r:(u + 1) * r])

    @pl.when(hub)
    def _():
        pl.semaphore_wait(told_sem, 1)
        for f in flips(final):
            pl.semaphore_signal(pair_sem, inc=1, device_id=neighbour(final, f), device_id_type=MESH)

    for h in reversed(late):
        give(COUP, h, [final])

    @pl.when(hub)
    def _():
        term_in(0, 1)
        n_out[1] = (t_out[0].astype(F32) + d_in[0, 1].astype(F32)).astype(BF16)

    landed(base, load_sem.at[3])
    for u in range(2):
        base[u * m:(u + 1) * m] = mm(da[u], db[u])
    pl.when(hub)(lambda: send_value(1))
    for h in range(2, levels - 1):
        give(COUP, h, down(COUP, h))
        give(DESC, h, down(DESC, h))
    for h in late:
        give(COUP, h, down(COUP, h)[1:])

    @pl.when(central)
    def _():
        for h in late:
            take(COUP, h)

    near[0] = mm(mm(coup[0, 0], leaf[1]), coup[0, 3])
    near[1] = mm(mm(coup[0, 1], leaf[0]), coup[0, 2])
    value_in(1)
    pl.when(hub)(lambda: landed(base.at[:2 * r * r // m], w_recv.at[place[COUP, 1]]))
    couple(cross[1], *factors(1, left_chain, right_chain))
    left_chain = mm(left_chain, desc[2, 0]).astype(BF16)
    right_chain = mm(right_chain, desc[2, 1]).astype(BF16)

    @pl.when(hub)
    def _():
        for h in range(2, levels - 1):
            take(ASC, h)
            if (SIB, h) in place:
                take(SIB, h)

    @pl.when(hub)
    def _():
        for g in range(1, final):
            lo, hi = groups[g]
            up_left = cols([weight(ASC, lo + 1, 0), weight(SIB, lo + 1, 0)])
            up_right = [weight(ASC, lo + 1, 1), weight(SIB, lo + 1, 1)]
            far_left = mm(weight(ASC, hi, 0), up_left).astype(BF16)
            far_right = mm(rows(up_right), weight(ASC, hi, 1))
            both = [cols([far_right[b * r:(b + 1) * r], up_right[b]]) for b in range(2)]
            here, there = ([1], [2, 3]) if g > 1 else ([4, 1, 5], [2, 6, 3, 7])
            landed(d_in.at[g, 1:1 + len(here + there)], term_sem(g, 1))
            own = sum((d_in[g, n].astype(F32) for n in here), t_out[g].astype(F32)).astype(BF16)
            other = sum(d_in[g, n].astype(F32) for n in there).astype(BF16)
            half = rows([mm(own, both[0]), mm(other, both[1])])
            t_out[g + 1] = mm(far_left, half[:, :r]).astype(BF16)
            if g + 1 == final:
                pl.semaphore_wait(pair_sem, len(upper))
                pl.when(ends)(lambda: send_term(final, 3, 1))
                send_term(final, 3)
                send_term(final, 2)
                send_term(final, 2, 1)
            else:
                for f in flips(g + 1):
                    send_term(g + 1, f)
            n_out[g + 1] = mm(up_left, half[:, r:]).astype(BF16)
            send_value(g + 1)
            if g + 1 == final:
                send_value(final, 1)
            cross[lo + 2] = other
            pass_value(lo + 2)
            value_in(lo + 1)
            pass_value(lo + 1)

    near_levels = range(2, late[0])
    landed(outer, load_sem.at[4])
    ready, chains = {}, {}
    for h in near_levels:
        if h > 2:
            if h > 3:
                take(DESC, h - 2)
            left_chain = mm(left_chain, weight(DESC, h - 2, 0)).astype(BF16)
            right_chain = mm(right_chain, weight(DESC, h - 2, 1)).astype(BF16)
        chains[h] = left_chain, right_chain
        if h < late[0] - 1:
            take(COUP, h)
            ready[h] = factors(h, *chains[h])
    if late[0] > 3:
        take(DESC, late[0] - 2)
    left_chain = mm(left_chain, weight(DESC, late[0] - 2, 0)).astype(BF16)
    right_chain = mm(right_chain, weight(DESC, late[0] - 2, 1)).astype(BF16)
    left_base = [mm(outer[u, 0], left_chain[u * r:(u + 1) * r]).astype(BF16) for u in range(2)]
    right_base = [mm(outer[u, 1], right_chain[u * r:(u + 1) * r]).astype(BF16) for u in range(2)]
    take(COUP, late[0] - 1)
    ready[late[0] - 1] = factors(late[0] - 1, *chains[late[0] - 1])

    @pl.when(side)
    def _():
        for h in near_levels:
            value_in(h)

    for h in near_levels:
        couple(cross[h], *ready[h])
    for u in range(2):
        base[u * m:(u + 1) * m] += mm(mm(outer[u, 0], near[u]), outer[u, 1], 1, 1)
    take(DESC, late[1] - 2)
    for h in late:
        take(COUP, h, jnp.logical_not(central))
    first = cols([weight(COUP, late[0], 0), mm(weight(DESC, late[1] - 2, 0), weight(COUP, late[1], 0))])
    second = rows([
        weight(COUP, late[0], 1),
        mm(weight(COUP, late[1], 1), weight(DESC, late[1] - 2, 1), 1, 1),
    ])
    for u in range(2):
        left[u] = mm(left_base[u], first).astype(BF16)
        right[u] = mm(second, right_base[u], 1, 1).astype(BF16)

    value_in(late[0])
    term_in(final, 2)
    term_in(final, 3)
    pl.when(hub & jnp.logical_not(ends))(lambda: pass_term(final, 3))

    ends_ref[0] = cross[late[0]]
    ends_ref[1] = (d_in[final, 2].astype(F32) + d_in[final, 3].astype(F32)).astype(BF16)

    rows_each = r * r // (2 * m)
    pl.when(side)(lambda: landed(base.at[:6 * rows_each], d_send.at[0]))
    pl.when(hub)(lambda: landed(base.at[:(1 + 6 * final) * rows_each], d_send.at[0]))
    for k in range(levels + 1):
        @pl.when(owner(k + 1) if k < levels else ones(levels))
        def _(k=k):
            units = 0
            for g in range(final + 1):
                for kind, h in place:
                    if g not in down(kind, h):
                        continue
                    if kind != SIB and g == top[h] and k == h - 1 or g < top[h] and k >= groups[g][1]:
                        units += len(targets(kind, h, g))
            unit = r * r // m
            while units:
                some = min(units, 2 * m // unit)
                landed(base.at[:some * unit], w_send.at[0])
                units -= some


def last_kernel(base, left, right, ends_ref, o_ref, result, sem):
    m = result.shape[1]
    near, far = ends_ref[0], ends_ref[1]
    zero = jnp.zeros_like(far)
    blocks = rows([cols([near, zero]), cols([zero, far])])
    spread = [mm(left[u], blocks).astype(BF16) for u in range(2)]
    copies = []
    for u in range(2):
        for n in range(4):
            part = slice(n * m // 4, (n + 1) * m // 4)
            start = u * m + n * m // 4
            result[u, part] = (base[start:start + m // 4] + mm(spread[u][part], right[u])).astype(BF16)
            copies.append(pltpu.make_async_copy(result.at[u, part], o_ref.at[u, part], sem.at[4 * u + n]))
            copies[-1].start()
    for copy in copies:
        copy.wait()


def shards(levels, columns, dense_a, dense_b, inner, outer, ascent, descent, couplings):
    r = ascent.shape[-1]
    m = dense_a.shape[-1]
    arrays = (dense_a, dense_b, inner, outer, ascent, descent, couplings)
    vmem = pltpu.VMEM
    dma = pltpu.SemaphoreType.DMA
    groups = split(levels)
    n = len(groups)
    parts = pl.pallas_call(
        functools.partial(tree_kernel, levels, columns),
        out_shape=(
            jax.ShapeDtypeStruct((2 * m, m), F32),
            jax.ShapeDtypeStruct((2, m, 2 * r), BF16),
            jax.ShapeDtypeStruct((2, 2 * r, m), BF16),
            jax.ShapeDtypeStruct((2, r, r), BF16),
        ),
        in_specs=[pl.BlockSpec(memory_space=pltpu.HBM)] * 7,
        out_specs=(pl.BlockSpec(memory_space=pltpu.VMEM),) * 4,
        scratch_shapes=[
            vmem(dense_a.shape, BF16),
            vmem(dense_b.shape, BF16),
            vmem(inner.shape, BF16),
            vmem(outer.shape, BF16),
            vmem(ascent.shape[1:], BF16),
            vmem(descent.shape[1:], BF16),
            vmem(couplings.shape[1:], BF16),
            vmem((len(kept(levels)), 2, r, r), BF16),
            vmem((n, r, r), BF16),
            vmem((n, r, r), BF16),
            vmem((n, 8, r, r), BF16),
            vmem((levels, r, r), BF16),
            vmem((2, r, r), F32),
            dma((5,)),
            dma((1,)),
            dma((len(kept(levels)),)),
            dma((1,)),
            dma((n + 1,)),
            dma((levels - 1,)),
            pltpu.SemaphoreType.REGULAR,
            pltpu.SemaphoreType.REGULAR,
        ],
        compiler_params=pltpu.CompilerParams(collective_id=0, has_side_effects=True, vmem_limit_bytes=24 * 2**20),
    )(*(pltpu.with_memory_space_constraint(x, pltpu.HBM) for x in arrays))
    return pl.pallas_call(
        last_kernel,
        out_shape=jax.ShapeDtypeStruct(dense_a.shape, BF16),
        in_specs=[pl.BlockSpec(memory_space=pltpu.VMEM)] * 4,
        out_specs=pl.BlockSpec(memory_space=pltpu.HBM),
        scratch_shapes=[vmem(dense_a.shape, BF16), dma((8,))],
        compiler_params=pltpu.CompilerParams(vmem_limit_bytes=8 * 2**20),
    )(*parts)


def solution(mesh):
    rows_, columns = mesh.shape["row"], mesh.shape["col"]
    levels = (rows_ * columns).bit_length() - 1
    both = ("row", "col")
    placed = (
        P(both, None, None),
        P(both, None, None),
        P(both, None, None, None),
        P(both, None, None, None),
        P(both, None, None, None, None),
        P(both, None, None, None, None),
        P(both, None, None, None, None),
    )
    return jax.shard_map(
        functools.partial(shards, levels, columns),
        mesh=mesh, in_specs=placed, out_specs=P(both, None, None), check_vma=False,
    )
```

```python
import functools

import jax
import jax.numpy as jnp
from jax import lax
from jax.experimental import pallas as pl
from jax.experimental.pallas import tpu as pltpu
from jax.sharding import PartitionSpec as P

MESH = pl.DeviceIdType.MESH
BF16 = jnp.bfloat16
F32 = jnp.float32
ASC, DESC, COUP, SIB = 0, 1, 2, 3


def mm(a, b, ca=1, cb=0):
    return lax.dot_general(
        a.astype(BF16), b.astype(BF16), (((ca,), (cb,)), ((), ())), preferred_element_type=F32
    )


def rows(values):
    return jnp.concatenate([v.astype(BF16) for v in values], 0)


def cols(values):
    return jnp.concatenate([v.astype(BF16) for v in values], 1)


def split(levels):
    cuts = [0, *range(1, levels + 1, 2)]
    return list(zip(cuts[:-1], cuts[1:]))


def kept(levels):
    groups = split(levels)
    firsts = [lo + 1 for lo, _ in groups[1:-1]]
    found = [(COUP, h) for h in range(1, levels + 1)]
    found += [(kind, h) for h in range(1, levels - 1) for kind in (ASC, DESC)]
    return found + [(SIB, h) for h in firsts]


def tree_kernel(
    levels, columns,
    da_ref, db_ref, inner_ref, outer_ref, asc_ref, desc_ref, coup_ref, base, left, right, ends_ref,
    da, db, inner, outer, asc, desc, coup,
    table, t_out, n_out, d_in, cross, near,
    load_sem, w_send, w_recv, d_send, d_recv, c_recv, told_sem, pair_sem,
):
    pos = lax.axis_index("row") * columns + lax.axis_index("col")
    bit = [pos // 2**i % 2 for i in range(levels)]
    groups = split(levels)
    final = len(groups) - 1
    top = {h: g for g, (lo, hi) in enumerate(groups) for h in range(lo + 1, hi + 1)}
    late = list(range(groups[final][0] + 1, levels + 1))
    r, m = asc.shape[-1], da.shape[-1]
    place = {item: n for n, item in enumerate(kept(levels))}

    def neighbour(g, f, core=0):
        lo, hi = groups[g]
        other = pos + core * (1 - 2 * bit[0])
        for i in range(lo, hi):
            if f >> (i - lo) & 1:
                other = other + 2**i * (1 - 2 * bit[i])
        return other // columns, other % columns

    def flips(g):
        lo, hi = groups[g]
        return [f for f in (1, 3, 2) if f < 2 ** (hi - lo)]

    def ones(n):
        return pos % 2**n == 2**n - 1

    def owner(h):
        return pos % 2**h == 2 ** (h - 1) - 1

    barrier = pltpu.get_barrier_semaphore()
    hub, side = ones(1), jnp.logical_not(ones(1))
    mate = neighbour(0, 1)
    lower = [neighbour(g, f) for g in range(1, final) for f in flips(g)]
    upper = [neighbour(final, f, 1) for f in flips(final)]

    def greet(others):
        for other in others:
            pl.semaphore_signal(barrier, inc=1, device_id=other, device_id_type=MESH)

    greet([mate])

    @pl.when(hub)
    def _():
        greet(lower)
        greet(upper)


    def load(src, dst, n):
        pltpu.make_async_copy(src, dst, load_sem.at[n]).start()

    def landed(ref, sem):
        pltpu.make_async_copy(ref, ref, sem).wait()

    load(asc_ref.at[0], asc, 0)
    load(inner_ref, inner, 1)

    def slot(kind, h):
        return table.at[place[kind, h]]

    def weight(kind, h, n):
        return table[place[kind, h], n]

    def targets(kind, h, g):
        lo, _ = groups[g]
        if g < top[h]:
            return [(f, kind, slot(kind, h)) for f in flips(g)]
        found = []
        for f in flips(g):
            beyond = f >> (h - lo)
            if kind == ASC:
                found.append((f, SIB if beyond else ASC, slot(ASC, h)))
            elif beyond:
                continue
            elif kind == COUP and f >> (h - 1 - lo) & 1:
                found.append((f, COUP, coup.at[1, 1:3]))
            else:
                found.append((f, kind, slot(kind, h)))
        return found

    def copies(kind, h, g):
        return [
            pltpu.make_async_remote_copy(
                src_ref=src, dst_ref=slot(to, h),
                send_sem=w_send.at[0], recv_sem=w_recv.at[place[COUP, 1] if (to, h) == (DESC, 1) else place[to, h]],
                device_id=neighbour(g, f), device_id_type=MESH,
            )
            for f, to, src in targets(kind, h, g)
        ]

    def give(kind, h, gs):
        @pl.when(owner(h))
        def _():
            for g in gs:
                for copy in copies(kind, h, g):
                    copy.start()

    def down(kind, h):
        return list(reversed(range(int(kind in (ASC, SIB) and h > 1), top[h] + 1)))

    def take(kind, h, who=None):
        waits = jnp.logical_not(owner(h)) if kind != SIB else None
        if who is not None:
            waits = who if waits is None else waits & who

        def body():
            pltpu.make_async_copy(slot(kind, h), slot(kind, h), w_recv.at[place[kind, h]]).wait()
            for g in [g for g in down(kind, h) if g < top[h]]:
                @pl.when(ones(groups[g][1]))
                def _(g=g):
                    for copy in copies(kind, h, g):
                        copy.start()

        if waits is None:
            body()
        else:
            pl.when(waits)(body)

    def remote(g, src, dst, recv, to):
        return pltpu.make_async_remote_copy(
            src_ref=src, dst_ref=dst, send_sem=d_send.at[0], recv_sem=recv,
            device_id=to, device_id_type=MESH,
        )

    def term_sem(g, f):
        return d_recv.at[g + int(g == final and f == 3)]

    def send_term(g, f, core=0):
        at = f + 4 * core if g == 1 else f
        remote(g, t_out.at[g], d_in.at[g, at], term_sem(g, f), neighbour(g, f, core)).start()

    def send_value(g, core=0):
        h = groups[g][0] + 1
        remote(g, n_out.at[g], cross.at[h], c_recv.at[h - 1], neighbour(g, 1, core)).start()

    def term_in(g, f):
        landed(d_in.at[g, f], term_sem(g, f))

    def value_in(h):
        landed(cross.at[h], c_recv.at[h - 1])

    def pass_value(h):
        remote(top[h], cross.at[h], cross.at[h], c_recv.at[h - 1], mate).start()

    def pass_term(g, f):
        remote(g, d_in.at[g, f], d_in.at[g, f], term_sem(g, f), mate).start()

    central = ones(groups[final][0])
    ends = bit[levels - 1] == bit[levels - 2]

    landed(asc, load_sem.at[0])
    for h in range(1, levels - 1):
        @pl.when(owner(h))
        def _(h=h):
            table[place[ASC, h], 0] = asc[3, 0].T
            table[place[ASC, h], 1] = asc[3, 1]

    def tell_mate():
        pl.semaphore_signal(told_sem, inc=1, device_id=mate, device_id_type=MESH)

    @pl.when(hub)
    def _():
        pl.semaphore_wait(barrier, 1 + len(lower))
        tell_mate()

    pl.when(side)(lambda: pl.semaphore_wait(told_sem, 1))
    for h in range(1, levels - 1):
        give(ASC, h, down(ASC, h))
    landed(inner, load_sem.at[1])
    load(coup_ref.at[0], coup, 2)
    load(desc_ref.at[0], desc, 2)
    load(da_ref, da, 3)
    load(db_ref, db, 3)
    load(outer_ref, outer, 4)
    turned = cols([asc[u, 0].T for u in range(2)])
    lifted_left = mm(asc[2, 0].T, turned).astype(BF16)
    lifted_right = mm(rows([asc[u, 1] for u in range(2)]), asc[2, 1])
    factors = [cols([asc[u, 1], lifted_right[u * r:(u + 1) * r]]) for u in range(2)]
    leaf = [mm(inner[u, 0], inner[u, 1], 0, 0).astype(BF16) for u in range(2)]
    half = rows([mm(leaf[u], factors[u]) for u in range(2)])
    term = mm(lifted_left, half[:, r:]).astype(BF16)
    n_out[0] = mm(turned, half[:, :r]).astype(BF16)
    t_out[0] = term
    pl.when(side)(lambda: send_term(0, 1))
    take(ASC, 1)
    t_out[1] = mm(weight(ASC, 1, 0), mm(term, weight(ASC, 1, 1))).astype(BF16)

    @pl.when(hub)
    def _():
        for f in (3, 1, 2):
            send_term(1, f)

    @pl.when(side)
    def _():
        for f in (3, 1, 2):
            send_term(1, f, 1)
        remote(1, t_out.at[1], d_in.at[1, 4], term_sem(1, 1), mate).start()

    send_value(0)
    landed(base.at[:16 * r * r // (2 * m)], load_sem.at[2])
    for h in reversed(range(1, levels + 1)):
        @pl.when(owner(h))
        def _(h=h):
            table[place[COUP, h], 0] = coup[1, 0]
            table[place[COUP, h], 1] = coup[1, 3]
            if h < levels - 1:
                table[place[DESC, h]] = desc[3]

        if h == 1:
            give(COUP, 1, [0])
            give(DESC, 1, [0])

    @pl.when(side)
    def _():
        pl.semaphore_wait(barrier, 1 + len(upper))
        tell_mate()

    left_chain = rows([desc[u, 0] for u in range(2)])
    right_chain = rows([desc[u, 1] for u in range(2)])

    def factors(h, left_chain, right_chain):
        before = mm(left_chain, weight(COUP, h, 0)).astype(BF16)
        return before, mm(weight(COUP, h, 1), right_chain, 1, 1).astype(BF16)

    def couple(value, before, after):
        spread = mm(value, after).astype(BF16)
        for u in range(2):
            near[u] += mm(before[u * r:(u + 1) * r], spread[:, u * r:(u + 1) * r])

    @pl.when(hub)
    def _():
        pl.semaphore_wait(told_sem, 1)
        for f in flips(final):
            pl.semaphore_signal(pair_sem, inc=1, device_id=neighbour(final, f), device_id_type=MESH)

    for h in reversed(late):
        give(COUP, h, [final])

    @pl.when(hub)
    def _():
        term_in(0, 1)
        n_out[1] = (t_out[0].astype(F32) + d_in[0, 1].astype(F32)).astype(BF16)

    landed(base, load_sem.at[3])
    for u in range(2):
        base[u * m:(u + 1) * m] = mm(da[u], db[u])
    pl.when(hub)(lambda: send_value(1))
    for h in range(2, levels - 1):
        give(COUP, h, down(COUP, h))
        give(DESC, h, down(DESC, h))
    for h in late:
        give(COUP, h, down(COUP, h)[1:])

    @pl.when(central)
    def _():
        for h in late:
            take(COUP, h)

    near[0] = mm(mm(coup[0, 0], leaf[1]), coup[0, 3])
    near[1] = mm(mm(coup[0, 1], leaf[0]), coup[0, 2])
    value_in(1)
    pl.when(hub)(lambda: landed(base.at[:2 * r * r // m], w_recv.at[place[COUP, 1]]))
    couple(cross[1], *factors(1, left_chain, right_chain))
    left_chain = mm(left_chain, desc[2, 0]).astype(BF16)
    right_chain = mm(right_chain, desc[2, 1]).astype(BF16)

    @pl.when(hub)
    def _():
        for h in range(2, levels - 1):
            take(ASC, h)
            if (SIB, h) in place:
                take(SIB, h)

    @pl.when(hub)
    def _():
        for g in range(1, final):
            lo, hi = groups[g]
            up_left = cols([weight(ASC, lo + 1, 0), weight(SIB, lo + 1, 0)])
            up_right = [weight(ASC, lo + 1, 1), weight(SIB, lo + 1, 1)]
            far_left = mm(weight(ASC, hi, 0), up_left).astype(BF16)
            far_right = mm(rows(up_right), weight(ASC, hi, 1))
            both = [cols([far_right[b * r:(b + 1) * r], up_right[b]]) for b in range(2)]
            here, there = ([1], [2, 3]) if g > 1 else ([4, 1, 5], [2, 6, 3, 7])
            landed(d_in.at[g, 1:1 + len(here + there)], term_sem(g, 1))
            own = sum((d_in[g, n].astype(F32) for n in here), t_out[g].astype(F32)).astype(BF16)
            other = sum(d_in[g, n].astype(F32) for n in there).astype(BF16)
            half = rows([mm(own, both[0]), mm(other, both[1])])
            t_out[g + 1] = mm(far_left, half[:, :r]).astype(BF16)
            if g + 1 == final:
                pl.semaphore_wait(pair_sem, len(upper))
                pl.when(ends)(lambda: send_term(final, 3, 1))
                send_term(final, 2, 1)
                send_term(final, 3)
                send_term(final, 2)
            else:
                for f in flips(g + 1):
                    send_term(g + 1, f)
            n_out[g + 1] = mm(up_left, half[:, r:]).astype(BF16)
            send_value(g + 1)
            if g + 1 == final:
                send_value(final, 1)
            cross[lo + 2] = other
            pass_value(lo + 2)
            value_in(lo + 1)
            pass_value(lo + 1)

    near_levels = range(2, late[0])
    landed(outer, load_sem.at[4])
    ready, chains = {}, {}
    for h in near_levels:
        if h > 2:
            if h > 3:
                take(DESC, h - 2)
            left_chain = mm(left_chain, weight(DESC, h - 2, 0)).astype(BF16)
            right_chain = mm(right_chain, weight(DESC, h - 2, 1)).astype(BF16)
        chains[h] = left_chain, right_chain
        if h < late[0] - 1:
            take(COUP, h)
            ready[h] = factors(h, *chains[h])
    if late[0] > 3:
        take(DESC, late[0] - 2)
    left_chain = mm(left_chain, weight(DESC, late[0] - 2, 0)).astype(BF16)
    right_chain = mm(right_chain, weight(DESC, late[0] - 2, 1)).astype(BF16)
    left_base = [mm(outer[u, 0], left_chain[u * r:(u + 1) * r]).astype(BF16) for u in range(2)]
    right_base = [mm(outer[u, 1], right_chain[u * r:(u + 1) * r]).astype(BF16) for u in range(2)]
    take(COUP, late[0] - 1)
    ready[late[0] - 1] = factors(late[0] - 1, *chains[late[0] - 1])

    @pl.when(side)
    def _():
        for h in near_levels:
            value_in(h)

    for h in near_levels:
        couple(cross[h], *ready[h])
    for u in range(2):
        base[u * m:(u + 1) * m] += mm(mm(outer[u, 0], near[u]), outer[u, 1], 1, 1)
    take(DESC, late[1] - 2)
    for h in late:
        take(COUP, h, jnp.logical_not(central))
    first = cols([weight(COUP, late[0], 0), mm(weight(DESC, late[1] - 2, 0), weight(COUP, late[1], 0))])
    second = rows([
        weight(COUP, late[0], 1),
        mm(weight(COUP, late[1], 1), weight(DESC, late[1] - 2, 1), 1, 1),
    ])
    for u in range(2):
        left[u] = mm(left_base[u], first).astype(BF16)
        right[u] = mm(second, right_base[u], 1, 1).astype(BF16)

    value_in(late[0])
    term_in(final, 2)
    term_in(final, 3)
    pl.when(hub & jnp.logical_not(ends))(lambda: pass_term(final, 3))

    ends_ref[0] = cross[late[0]]
    ends_ref[1] = (d_in[final, 2].astype(F32) + d_in[final, 3].astype(F32)).astype(BF16)

    rows_each = r * r // (2 * m)
    pl.when(side)(lambda: landed(base.at[:6 * rows_each], d_send.at[0]))
    pl.when(hub)(lambda: landed(base.at[:(1 + 6 * final) * rows_each], d_send.at[0]))
    for k in range(levels + 1):
        @pl.when(owner(k + 1) if k < levels else ones(levels))
        def _(k=k):
            units = 0
            for g in range(final + 1):
                for kind, h in place:
                    if g not in down(kind, h):
                        continue
                    if kind != SIB and g == top[h] and k == h - 1 or g < top[h] and k >= groups[g][1]:
                        units += len(targets(kind, h, g))
            unit = r * r // m
            while units:
                some = min(units, 2 * m // unit)
                landed(base.at[:some * unit], w_send.at[0])
                units -= some


def last_kernel(base, left, right, ends_ref, o_ref, result, sem):
    m = result.shape[1]
    near, far = ends_ref[0], ends_ref[1]
    zero = jnp.zeros_like(far)
    blocks = rows([cols([near, zero]), cols([zero, far])])
    spread = [mm(left[u], blocks).astype(BF16) for u in range(2)]
    copies = []
    for u in range(2):
        for n in range(4):
            part = slice(n * m // 4, (n + 1) * m // 4)
            start = u * m + n * m // 4
            result[u, part] = (base[start:start + m // 4] + mm(spread[u][part], right[u])).astype(BF16)
            copies.append(pltpu.make_async_copy(result.at[u, part], o_ref.at[u, part], sem.at[4 * u + n]))
            copies[-1].start()
    for copy in copies:
        copy.wait()


def shards(levels, columns, dense_a, dense_b, inner, outer, ascent, descent, couplings):
    r = ascent.shape[-1]
    m = dense_a.shape[-1]
    arrays = (dense_a, dense_b, inner, outer, ascent, descent, couplings)
    vmem = pltpu.VMEM
    dma = pltpu.SemaphoreType.DMA
    groups = split(levels)
    n = len(groups)
    parts = pl.pallas_call(
        functools.partial(tree_kernel, levels, columns),
        out_shape=(
            jax.ShapeDtypeStruct((2 * m, m), F32),
            jax.ShapeDtypeStruct((2, m, 2 * r), BF16),
            jax.ShapeDtypeStruct((2, 2 * r, m), BF16),
            jax.ShapeDtypeStruct((2, r, r), BF16),
        ),
        in_specs=[pl.BlockSpec(memory_space=pltpu.HBM)] * 7,
        out_specs=(pl.BlockSpec(memory_space=pltpu.VMEM),) * 4,
        scratch_shapes=[
            vmem(dense_a.shape, BF16),
            vmem(dense_b.shape, BF16),
            vmem(inner.shape, BF16),
            vmem(outer.shape, BF16),
            vmem(ascent.shape[1:], BF16),
            vmem(descent.shape[1:], BF16),
            vmem(couplings.shape[1:], BF16),
            vmem((len(kept(levels)), 2, r, r), BF16),
            vmem((n, r, r), BF16),
            vmem((n, r, r), BF16),
            vmem((n, 8, r, r), BF16),
            vmem((levels, r, r), BF16),
            vmem((2, r, r), F32),
            dma((5,)),
            dma((1,)),
            dma((len(kept(levels)),)),
            dma((1,)),
            dma((n + 1,)),
            dma((levels - 1,)),
            pltpu.SemaphoreType.REGULAR,
            pltpu.SemaphoreType.REGULAR,
        ],
        compiler_params=pltpu.CompilerParams(collective_id=0, has_side_effects=True, vmem_limit_bytes=24 * 2**20),
    )(*(pltpu.with_memory_space_constraint(x, pltpu.HBM) for x in arrays))
    return pl.pallas_call(
        last_kernel,
        out_shape=jax.ShapeDtypeStruct(dense_a.shape, BF16),
        in_specs=[pl.BlockSpec(memory_space=pltpu.VMEM)] * 4,
        out_specs=pl.BlockSpec(memory_space=pltpu.HBM),
        scratch_shapes=[vmem(dense_a.shape, BF16), dma((8,))],
        compiler_params=pltpu.CompilerParams(vmem_limit_bytes=8 * 2**20),
    )(*parts)


def solution(mesh):
    rows_, columns = mesh.shape["row"], mesh.shape["col"]
    levels = (rows_ * columns).bit_length() - 1
    both = ("row", "col")
    placed = (
        P(both, None, None),
        P(both, None, None),
        P(both, None, None, None),
        P(both, None, None, None),
        P(both, None, None, None, None),
        P(both, None, None, None, None),
        P(both, None, None, None, None),
    )
    return jax.shard_map(
        functools.partial(shards, levels, columns),
        mesh=mesh, in_specs=placed, out_specs=P(both, None, None), check_vma=False,
    )
```
